32 devices in a mesh: groups: 2 (over y), ctx: 4 (over z), tp: 4 (over x, core).
Axes of the slice: x: 2, y: 2, z: 4, core: 2. Of those that a mesh axis runs over, the one named last changes fastest.
Arguments:
- q_nope: bfloat16 [512, 16384], P(('groups', 'ctx'), 'tp'), parts along dimension 0, may hold values from -6 to 6
- q_rope: bfloat16 [512, 8192], P(('groups', 'ctx'), 'tp'), parts along dimension 0, may hold values from -6 to 6
- c_kv: bfloat16 [512, 512], P(('groups', 'ctx')), parts along dimension 0, may hold values from -6 to 46.4
- k_rope: bfloat16 [512, 64], P(('groups', 'ctx')), parts along dimension 0, may hold values from -6 to 6
- positions: int32 [512], P(('groups', 'ctx')), parts along dimension 0, may hold values from 0 to 255, as said below
- w_uk: bfloat16 [128, 128, 512], P('tp', 'ctx'), may hold values from -0.5 to 0.5
- w_uv: bfloat16 [128, 512, 128], P('tp', 'ctx'), may hold values from -0.25 to 0.25
- w_out: bfloat16 [16384, 7168], P('tp', 'ctx'), may hold values from -0.125 to 0.125
Outputs:
- attn_proj: bfloat16 [512, 7168], P(('groups', 'tp'), 'ctx'), parts along dimension 0
The draws below stay inside these ranges and needn't reach their ends.
There are 2 independent parts, one for each index of `groups`. The reference program is written for one: setup_inputs(seed, part) draws one part's arguments, and reference() takes and returns one part's arrays. A program takes and returns all parts, laid end to end along the dimension named above; an argument that names none is the same for every part. Nothing has to cross between parts.
Inputs may be any that keep to these rules, and one draw needn't show every extreme that they name: The positions are the 256 integers 0 to 255, each once; every aligned block of 32 rows holds consecutive ascending positions.
All inputs are finite; a program needn't handle non-finite values.
Results may differ from the reference program's by a relative error of at most 0.015.
Values may be sent and summed in bfloat16 or wider, within the bound.
A program may use at most 64 MiB of HBM per device.

```python
import jax
import jax.numpy as jnp
from jax import lax

D = 7168
HEADS = 128
LAT = 512
ROPE = 64
NOPE = 128
VDIM = 128
TOK_DEV = 64
SEQ = 256


def draw_c_kv(key, part):
    latent = jnp.clip(jax.random.normal(key, (SEQ, LAT), jnp.float32), -6.0, 6.0)
    return latent.astype(jnp.bfloat16)


def draw_positions(key, part):
    half_len = TOK_DEV // 2
    block_count = SEQ // half_len
    order = jax.random.permutation(jax.random.fold_in(key, 11), block_count)
    grid = order[:, None].astype(jnp.int32) * half_len + jnp.arange(half_len, dtype=jnp.int32)[None, :]
    return grid.reshape(SEQ).astype(jnp.int32)


def block_scale(rng, dims, cuts, low, top_value):
    def one(dim, parts):
        draws = jax.random.uniform(jax.random.fold_in(jax.random.fold_in(rng, 6), dim), (parts,), jnp.float32, low / len(cuts), top_value / len(cuts))
        return jnp.repeat(jnp.exp(draws), dims[dim] // parts).reshape((-1,) + (1,) * (len(dims) - dim - 1))

    loudness = one(*cuts[0])
    for cut in cuts[1:]:
        loudness = loudness * one(*cut)
    return loudness


def scatter_about(key, shape, width, reach, pieces=(), kind=jnp.bfloat16):
    array = jax.random.normal(key, shape, jnp.float32) * width
    if len(pieces) > 0:
        array = block_scale(key, shape, pieces, -0.22, 0.18) * array
    return jnp.clip(array, min=-reach, max=reach).astype(kind)


def setup_inputs(seed: int = 0, part: int = 0) -> dict:
    splits = jax.random.split(jax.random.key(seed), 9)
    own_keys = jax.random.split(jax.random.fold_in(splits[8], part), 9)
    q_nope = scatter_about(own_keys[0], (SEQ, HEADS * NOPE), 1.0, 6.0, ((0, 4), (1, 4)))
    q_rope = scatter_about(own_keys[1], (SEQ, HEADS * ROPE), 1.0, 6.0, ((0, 4), (1, 4)))
    c_kv = draw_c_kv(jax.random.fold_in(jax.random.fold_in(splits[8], part), 71), part)
    k_rope = scatter_about(own_keys[3], (SEQ, ROPE), 1.0, 6.0, ((0, 4),))
    positions = draw_positions(jax.random.fold_in(jax.random.fold_in(splits[8], part), 71), part)
    w_uk = scatter_about(splits[5], (HEADS, NOPE, LAT), NOPE ** -0.5, 0.5, ((0, 4), (1, 4)))
    w_uv = scatter_about(splits[6], (HEADS, LAT, VDIM), LAT ** -0.5, 0.25, ((0, 4), (1, 4)))
    w_out = scatter_about(splits[7], (HEADS * VDIM, D), (HEADS * VDIM // 8) ** -0.5, 0.125, ((0, 4), (1, 4)))
    return {"q_nope": q_nope, "q_rope": q_rope, "c_kv": c_kv, "k_rope": k_rope, "positions": positions, "w_uk": w_uk, "w_uv": w_uv, "w_out": w_out}


def rotate(values, position):
    half_dim = values.shape[-1] // 2
    freqs = 10000.0 ** (-jnp.arange(half_dim, dtype=jnp.float32) / half_dim)
    angles = position.astype(jnp.float32)[..., None] * freqs
    cosine = jnp.cos(angles)
    sine = jnp.sin(angles)
    first_half = values[..., :half_dim].astype(jnp.float32)
    second_half = values[..., half_dim:].astype(jnp.float32)
    return jnp.concatenate([first_half * cosine - second_half * sine, second_half * cosine + first_half * sine], axis=-1)


def reference(q_nope, q_rope, c_kv, k_rope, positions, w_uk, w_uv, w_out):
    softmax_scale = (NOPE + ROPE) ** -0.5
    q_parts = q_nope.reshape(SEQ, HEADS, NOPE).astype(jnp.float32)
    q_lat = jnp.einsum("thn,hnl->htl", q_parts, w_uk.astype(jnp.float32)).astype(jnp.bfloat16)
    q_rot = rotate(q_rope.reshape(SEQ, HEADS, ROPE), positions[:, None]).astype(jnp.bfloat16)
    q_rot = jnp.transpose(q_rot, (1, 0, 2))
    k_rot = rotate(k_rope, positions).astype(jnp.bfloat16)
    key_rows = jnp.concatenate([c_kv, k_rot], axis=1)
    visible = positions[None, :] <= positions[:, None]

    def one_head(operands):
        lat_part, rot_part = operands
        queries = jnp.concatenate([lat_part, rot_part], axis=1)
        scores = jnp.dot(queries, key_rows.T, preferred_element_type=jnp.float32) * softmax_scale
        row_max = jnp.max(jnp.where(visible, scores, -1e30), axis=1)
        weights = jnp.where(visible, jnp.exp(scores - row_max[:, None]), 0.0)
        total = jnp.sum(weights, axis=1)
        mixed = jnp.dot(weights.astype(jnp.bfloat16), c_kv, preferred_element_type=jnp.float32)
        return (mixed / total[:, None]).astype(jnp.bfloat16)

    o_lat = lax.map(one_head, (q_lat, q_rot))
    head_out = jnp.einsum("hsl,hlv->shv", o_lat.astype(jnp.float32), w_uv.astype(jnp.float32))
    head_out = head_out.astype(jnp.bfloat16).reshape(SEQ, HEADS * VDIM)
    return jnp.dot(head_out, w_out, preferred_element_type=jnp.float32).astype(jnp.bfloat16)
```

```python
import functools
import math

import jax
import jax.numpy as jnp
from jax import lax
from jax.experimental import pallas as pl
from jax.experimental.pallas import tpu as pltpu
from jax.sharding import PartitionSpec as P

F32 = jnp.float32
BF16 = jnp.bfloat16
MESH = pl.DeviceIdType.MESH


def rotate(values, position):
    half_dim = values.shape[-1] // 2
    freqs = 10000.0 ** (-jnp.arange(half_dim, dtype=jnp.float32) / half_dim)
    angles = position.astype(jnp.float32)[..., None] * freqs
    cosine = jnp.cos(angles)
    sine = jnp.sin(angles)
    first_half = values[..., :half_dim].astype(jnp.float32)
    second_half = values[..., half_dim:].astype(jnp.float32)
    return jnp.concatenate(
        [first_half * cosine - second_half * sine, second_half * cosine + first_half * sine],
        axis=-1,
    )


def mega(sz, qn_in, qr_in, kv_in, kr_in, pos_in, wuk_in, wuv_in, wout_in, out_ref,
         qn, qr, kv, kr, pos, wuk, wuv, wout, krot, table, limit, ho, acc, part, got,
         s1, r1, sy, ry, st, rt, s_right, s_left, r_ag, s_rs, r_rs, loc, loc_out):
    n, groups, tps, ends, mids = sz["n"], sz["g"], sz["t"], sz["ends"], sz["mids"]
    tok, hc, nope, rope, lat, vdim = (sz[k] for k in ("tok", "hc", "nope", "rope", "lat", "vdim"))
    scale = (nope + rope) ** (-0.5)
    hg = hc // groups
    c = lax.axis_index("ctx")
    g = lax.axis_index("groups")
    t = lax.axis_index("tp")
    nsl = nope // n
    lsl = lat // n
    share = tok // tps
    seq = n * tok

    def outer(j):
        return jnp.logical_or(j == 0, j == n - 1)

    def count(j):
        return jnp.where(outer(j), ends, mids)

    def begin(j):
        return jnp.where(j == 0, 0, ends + (j - 1) * mids)

    mine = count(c)
    first_mine = begin(c)
    at_end = outer(c)

    barrier = pltpu.get_barrier_semaphore()
    for axis, me, size in (("ctx", c, n), ("groups", g, groups), ("tp", t, tps)):
        for d in range(1, size):
            pl.semaphore_signal(barrier, inc=1, device_id={axis: lax.rem(me + d, size)}, device_id_type=MESH)
    pl.semaphore_wait(barrier, (n - 1) + (groups - 1) + (tps - 1))

    def al(x, m):
        return pl.multiple_of(x, m)

    def guard(i, j, body):
        if i < ends:
            body()
        else:
            pl.when(jnp.logical_not(outer(j)))(body)

    def rows_of(s):
        return pl.ds(al(s * tok, tok), tok)

    def piece(kind, i, j, s, part_of):
        if kind in (0, 5):
            src, dst = (kv_in, kv) if kind == 0 else (kr_in, kr)
            if part_of is None:
                return src, dst.at[rows_of(s), :]
            return (src.at[pl.ds(al(part_of * share, share), share), :],
                    dst.at[pl.ds(al(s * tok + part_of * share, share), share), :])
        if kind == 6:
            return pos_in, pos.at[s]
        if kind == 1:
            w = hc * nope
            return (qn_in.at[:, pl.ds(al((begin(j) + i) * w, w), w)],
                    qn.at[rows_of(s), pl.ds(i * w, w)])
        if kind == 2:
            w = hc * rope
            return (qr_in.at[:, pl.ds(al((begin(j) + i) * w, w), w)],
                    qr.at[rows_of(s), pl.ds(i * w, w)])
        if part_of is None:
            src_h, dst_h = pl.ds((begin(j) + i) * hc, hc), pl.ds(i * hc, hc)
        else:
            src_h = pl.ds((begin(j) + i) * hc + part_of * hg, hg)
            dst_h = pl.ds(i * hc + part_of * hg, hg)
        if kind == 3:
            return wuk_in.at[src_h], wuk.at[dst_h, pl.ds(al(s * nsl, nsl), nsl), :]
        return wuv_in.at[src_h], wuv.at[dst_h, pl.ds(al(s * lsl, lsl), lsl), :]

    def copy1(kind, i, d, sending):
        owner = t if kind in (0, 5) else g
        if sending:
            j = lax.rem(c + d, n)
            src, dst = piece(kind, i, j, c, owner)
        else:
            j = lax.rem(c + n - d, n)
            src, dst = piece(kind, i, c, j, owner)
        return pltpu.make_async_remote_copy(
            src_ref=src, dst_ref=dst, send_sem=s1.at[kind, i, d - 1], recv_sem=r1.at[kind, i, d - 1],
            device_id={"ctx": j}, device_id_type=MESH)

    def local(kind, i):
        src, dst = piece(kind, i, c, c, None)
        return pltpu.make_async_copy(src, dst, loc.at[kind, i])

    def kinds(i):
        return (0, 1, 2, 3, 4, 5, 6) if i == 0 else (1, 2, 3, 4)

    def issue(i, group):
        for d in range(n - 1, 0, -1):
            def go():
                for kind in group:
                    copy1(kind, i, d, True).start()
            guard(i, lax.rem(c + d, n), go)

    def issue_chunk(i):
        issue(i, (3, 4))
        issue(i, (1, 2))

    issue(0, (6, 0, 5))
    window = sz["window"]
    for i in range(mids):
        if i < window:
            issue_chunk(i)
        else:
            pl.when(at_end)(functools.partial(issue_chunk, i))
    for i in range(mids):
        def go():
            for kind in kinds(i):
                local(kind, i).start()
        guard(i, c, go)
    wout_copy = pltpu.make_async_copy(wout_in, wout, loc_out)
    wout_copy.start()

    def copy_y(kind, i, e, d, sending):
        s = lax.rem(c + n - d, n)
        owner = g if sending else lax.rem(g + groups - e, groups)
        _, dst = piece(kind, i, c, s, owner)
        to = lax.rem(g + e, groups) if sending else owner
        return pltpu.make_async_remote_copy(
            src_ref=dst, dst_ref=dst, send_sem=sy.at[kind - 3, i, e - 1, d - 1],
            recv_sem=ry.at[kind - 3, i, e - 1, d - 1],
            device_id={"groups": to}, device_id_type=MESH)

    def copy_t(kind, e, d, sending):
        s = lax.rem(c + n - d, n)
        owner = t if sending else lax.rem(t + tps - e, tps)
        _, dst = piece(kind, 0, c, s, owner)
        to = lax.rem(t + e, tps) if sending else owner
        return pltpu.make_async_remote_copy(
            src_ref=dst, dst_ref=dst, send_sem=st.at[kind // 5, e - 1, d - 1],
            recv_sem=rt.at[kind // 5, e - 1, d - 1],
            device_id={"tp": to}, device_id_type=MESH)

    def forward_weights(i):
        for kind in (3, 4):
            for d in range(1, n):
                copy1(kind, i, d, False).wait_recv()
                for e in range(1, groups):
                    copy_y(kind, i, e, d, True).start()

    def forward_keys():
        for d in range(1, n):
            for kind in (0, 5):
                copy1(kind, 0, d, False).wait_recv()
                for e in range(1, tps):
                    copy_t(kind, e, d, True).start()

    wide = 2 * rope

    def turn(x):
        lane = lax.broadcasted_iota(jnp.int32, x.shape, 1)
        low = lax.rem(lane, rope) < rope // 2
        other = jnp.where(low, -pltpu.roll(x, wide - rope // 2, 1), pltpu.roll(x, rope // 2, 1))
        return x * table[0] + other * table[1]

    def tables():
        for d in range(1, n):
            copy1(6, 0, d, False).wait_recv()
        local(6, 0).wait()
        row = jnp.concatenate([pos[s] for s in range(n)], axis=1).astype(F32)
        col = jnp.broadcast_to(row, (wide, seq)).T
        lane = lax.broadcasted_iota(jnp.int32, (1, wide), 1)
        index = lax.rem(lane, rope // 2).astype(F32)
        freqs = jnp.exp(index * (-math.log(10000.0) / (rope // 2)))
        angles = col * freqs
        table[0] = jnp.cos(angles)
        table[1] = jnp.sin(angles)
        limit[...] = jnp.where(row > col[:, :1], -1e30, 3e38)

    def keys():
        for kind in (0, 5):
            local(kind, 0).wait()
            for e in range(1, tps):
                for d in range(1, n):
                    copy_t(kind, e, d, False).wait_recv()
        raw = kr[...].astype(F32)
        turned = turn(jnp.concatenate([raw, raw], axis=1))
        lane = lax.broadcasted_iota(jnp.int32, turned.shape, 1)
        krot[0] = jnp.where(lane < rope, turned, 0.0).astype(BF16)
        krot[1] = jnp.where(lane < rope, 0.0, turned).astype(BF16)

    def attend(i):
        nt = (((1,), (1,)), ((), ()))

        def pair(p, carry):
            raw = qr[:, pl.ds(al((i * (hc // 2) + p) * wide, wide), wide)]
            qrp = turn(raw.astype(F32)).astype(BF16)
            for k in range(2):
                hl = 2 * p + k
                h = i * hc + hl
                q = qn[:, pl.ds(al(h * nope, nope), nope)]
                ql = jnp.dot(q, wuk[h], preferred_element_type=F32).astype(BF16)
                sc = lax.dot_general(ql, kv[...], nt, preferred_element_type=F32)
                sc = (sc + lax.dot_general(qrp, krot[k], nt, preferred_element_type=F32)) * scale
                sc = jnp.minimum(sc, limit[...])
                w = jnp.exp(sc - jnp.max(sc, axis=1, keepdims=True))
                total = jnp.sum(w, axis=1, keepdims=True)
                o = jnp.dot(w.astype(BF16), kv[...], preferred_element_type=F32)
                o = (o / total).astype(BF16)
                ho[first_mine + i, :, pl.ds(al(hl * vdim, vdim), vdim)] = jnp.dot(
                    o, wuv[h], preferred_element_type=F32).astype(BF16)
            return carry

        lax.fori_loop(0, hc // 2, pair, 0)

    away, stay = 0, 1
    half_rows = seq // 2
    side = t // 2

    def rows_half(h):
        return pl.ds(al((1 - side if h == away else side) * half_rows, half_rows), half_rows)

    def ag_copy(q, h, right):
        ref = ho.at[q, rows_half(h), :]
        return pltpu.make_async_remote_copy(
            src_ref=ref, dst_ref=ref, send_sem=(s_right if right else s_left).at[q, h],
            recv_sem=r_ag.at[q, h],
            device_id={"ctx": c + 1 if right else c - 1}, device_id_type=MESH)

    inner_right = c < n // 2

    def send_inward(i, h):
        pl.when(inner_right)(lambda: ag_copy(first_mine + i, h, True).start())
        pl.when(jnp.logical_not(inner_right))(lambda: ag_copy(first_mine + i, h, False).start())

    def send_outward(i, h):
        pl.when(jnp.logical_and(inner_right, c > 0))(
            lambda: ag_copy(first_mine + i, h, False).start())
        pl.when(jnp.logical_and(jnp.logical_not(inner_right), c + 1 < n))(
            lambda: ag_copy(first_mine + i, h, True).start())

    cols = acc.shape[1]
    tile = sz["tile"]
    kdim = hc * vdim

    def project(q, rows, first=False):
        depth = pl.ds(al(q * kdim, kdim), kdim)

        def step(j, carry):
            at = pl.ds(al(j * tile, tile), tile)
            value = jnp.dot(ho[q, rows, :], wout[depth, at], preferred_element_type=F32)
            acc[rows, at] = value if first else acc[rows, at] + value
            return carry

        lax.fori_loop(0, cols // tile, step, 0)

    def handle(d, i, h):
        @pl.when(jnp.logical_and(c + d < n, i < count(c + d)))
        def _():
            q = begin(c + d) + i
            ag_copy(q, h, False).wait_recv()
            pl.when(c > 0)(lambda: ag_copy(q, h, False).start())
            project(q, rows_half(h))

        @pl.when(jnp.logical_and(c - d >= 0, i < count(c - d)))
        def _():
            q = begin(c - d) + i
            ag_copy(q, h, True).wait_recv()
            pl.when(c + 1 < n)(lambda: ag_copy(q, h, True).start())
            project(q, rows_half(h))

    def handle_all(d, low, high, h):
        def body(i, carry):
            handle(d, i, h)
            return carry

        lax.fori_loop(low, high, body, 0)

    early = sz["early"]

    def chunk(i):
        for kind in (1, 2):
            for d in range(1, n):
                copy1(kind, i, d, False).wait_recv()
        for kind in (1, 2, 3, 4):
            local(kind, i).wait()
        for kind in (3, 4):
            for e in range(1, groups):
                for d in range(1, n):
                    copy_y(kind, i, e, d, False).wait_recv()
        attend(i)
        if i + window < mids:
            pl.when(jnp.logical_not(at_end))(functools.partial(issue_chunk, i + window))
        send_outward(i, away)
        send_inward(i, away)
        send_outward(i, stay)
        if i < early:
            send_inward(i, stay)
        if i == 0:
            wout_copy.wait()
        project(first_mine + i, slice(None), i == 0)
        if i > 0:
            handle(1, i - 1, away)
            if i - 1 < early:
                handle(1, i - 1, stay)

    forward_keys()
    forward_weights(0)
    tables()
    keys()
    for i in range(mids):
        if i + 1 < mids:
            guard(i + 1, c, functools.partial(forward_weights, i + 1))
        guard(i, c, functools.partial(chunk, i))

    def send_late():
        for i in range(early, mids):
            guard(i, c, functools.partial(send_inward, i, stay))

    pl.when(at_end)(send_late)
    handle_all(1, mine - 1, mids, away)
    pl.when(jnp.logical_not(at_end))(send_late)

    rows_out = out_ref.shape[0]
    half = cols // 2
    core = lax.rem(t, 2)
    mate = t + 1 - 2 * core
    across = lax.rem(t + 2, tps)
    mate_across = lax.rem(mate + 2, tps)

    def block(r, at):
        return acc[pl.ds(al(r * rows_out, rows_out), rows_out), at]

    def rs_copy(stage, k):
        at = pl.ds(k * half, half)
        slot = (1, 2, 0)[stage]
        return pltpu.make_async_remote_copy(
            src_ref=part.at[slot, :, at], dst_ref=got.at[slot, :, at],
            send_sem=s_rs.at[stage, k], recv_sem=r_rs.at[stage, k],
            device_id={"tp": across if stage == 1 else mate}, device_id_type=MESH)

    spans = [slice(k * half, (k + 1) * half) for k in range(2)]

    handle_all(2, 0, mids, away)
    for i in range(mids):
        def done():
            for kind in (3, 4):
                for e in range(1, groups):
                    for d in range(1, n):
                        copy_y(kind, i, e, d, True).wait_send()
        guard(i, c, done)
    handle_all(3, 0, ends, away)
    for k, at in enumerate(spans):
        part[1, :, at] = block(mate_across, at).astype(BF16)
        rs_copy(0, k).start()
    handle(1, early, stay)
    for k, at in enumerate(spans):
        rs_copy(0, k).wait_recv()
        part[2, :, at] = (block(across, at) + got[1, :, at].astype(F32)).astype(BF16)
        rs_copy(1, k).start()
    handle_all(1, early + 1, mids, stay)
    for i in range(mids):
        for d in range(1, n):
            def done():
                for kind in kinds(i):
                    copy1(kind, i, d, True).wait_send()
            guard(i, lax.rem(c + d, n), done)
    for kind in (0, 5):
        for e in range(1, tps):
            for d in range(1, n):
                copy_t(kind, e, d, True).wait_send()
    handle_all(2, 0, mids, stay)

    def drain(h):
        def right(q, carry):
            ag_copy(q, h, True).wait_send()
            return carry

        def left(q, carry):
            ag_copy(q, h, False).wait_send()
            return carry

        pl.when(c + 1 < n)(lambda: lax.fori_loop(0, first_mine + mine, right, None))
        pl.when(c > 0)(lambda: lax.fori_loop(first_mine, ho.shape[0], left, None))

    drain(away)
    handle_all(3, 0, ends, stay)
    for k, at in enumerate(spans):
        part[0, :, at] = block(mate, at).astype(BF16)
        rs_copy(2, k).start()
    drain(stay)
    for k, at in enumerate(spans):
        rs_copy(1, k).wait_recv()
        own = block(t, at) + got[2, :, at].astype(F32)
        rs_copy(2, k).wait_recv()
        out_ref[:, at] = (own + got[0, :, at].astype(F32)).astype(BF16)
    for stage in range(3):
        for k in range(2):
            rs_copy(stage, k).wait_send()


def fast(sz, q_nope, q_rope, c_kv, k_rope, positions, w_uk, w_uv, w_out):
    n, groups, tps, ends, mids = sz["n"], sz["g"], sz["t"], sz["ends"], sz["mids"]
    tok, hc, nope, rope, lat, vdim = (sz[k] for k in ("tok", "hc", "nope", "rope", "lat", "vdim"))
    heads = w_uk.shape[0]
    chunks = heads // hc
    hpc = mids * hc
    seq = n * tok
    cols = w_out.shape[1]
    hbm = pl.BlockSpec(memory_space=pltpu.HBM)
    dma = pltpu.SemaphoreType.DMA
    more = max(groups - 1, 1)
    return pl.pallas_call(
        functools.partial(mega, sz),
        out_shape=jax.ShapeDtypeStruct((seq // tps, cols), BF16),
        in_specs=[hbm] * 8,
        out_specs=pl.BlockSpec(memory_space=pltpu.VMEM),
        scratch_shapes=[
            pltpu.VMEM((seq, hpc * nope), BF16),
            pltpu.VMEM((seq, hpc * rope), BF16),
            pltpu.VMEM((seq, lat), BF16),
            pltpu.VMEM((seq, rope), BF16),
            pltpu.VMEM((n, 1, tok), jnp.int32),
            pltpu.VMEM((hpc, nope, lat), BF16),
            pltpu.VMEM((hpc, lat, vdim), BF16),
            pltpu.VMEM(w_out.shape, BF16),
            pltpu.VMEM((2, seq, 2 * rope), BF16),
            pltpu.VMEM((2, seq, 2 * rope), F32),
            pltpu.VMEM((seq, seq), F32),
            pltpu.VMEM((chunks, seq, hc * vdim), BF16),
            pltpu.VMEM((seq, cols), F32),
            pltpu.VMEM((tps - 1, seq // tps, cols), BF16),
            pltpu.VMEM((tps - 1, seq // tps, cols), BF16),
            dma((7, mids, n - 1)),
            dma((7, mids, n - 1)),
            dma((2, mids, more, n - 1)),
            dma((2, mids, more, n - 1)),
            dma((2, tps - 1, n - 1)),
            dma((2, tps - 1, n - 1)),
            dma((chunks, 2)),
            dma((chunks, 2)),
            dma((chunks, 2)),
            dma((3, 2)),
            dma((3, 2)),
            dma((7, mids)),
            dma,
        ],
        compiler_params=pltpu.CompilerParams(collective_id=0, has_side_effects=True,
                                             vmem_limit_bytes=60 * 1024 * 1024),
    )(q_nope, q_rope, c_kv, k_rope, positions.reshape(1, tok), w_uk, w_uv, w_out)


def general(q_nope, q_rope, c_kv, k_rope, positions, w_uk, w_uv, w_out):
    tok_count = q_nope.shape[0]
    head_count = w_uk.shape[0]
    latent = c_kv.shape[1]
    up_key, up_value = (
        lax.all_gather(w_uk, "ctx", axis=1, tiled=True),
        lax.all_gather(w_uv, "ctx", axis=1, tiled=True),
    )
    nope_dim = up_key.shape[1]
    rope_dim = k_rope.shape[1]
    softmax_scale = (nope_dim + rope_dim) ** (-0.5)
    q_parts = q_nope.reshape(tok_count, head_count, nope_dim)
    q_lat = jnp.einsum("thn,hnl->thl", q_parts, up_key, preferred_element_type=jnp.float32).astype(
        jnp.bfloat16
    )
    q_rot = rotate(q_rope.reshape(tok_count, head_count, rope_dim), positions[:, None]).astype(
        jnp.bfloat16
    )
    k_rot = rotate(k_rope, positions).astype(jnp.bfloat16)
    key_rows = jnp.concatenate([c_kv, k_rot], axis=1)
    queries = jnp.concatenate([q_lat, q_rot], axis=2).reshape(
        tok_count * head_count, latent + rope_dim
    )
    query_pos = jnp.repeat(positions, head_count)
    row_total = tok_count * head_count
    key_part = lax.all_gather(key_rows, "ctx", axis=0, tiled=True)
    key_pos = lax.all_gather(positions, "ctx", axis=0, tiled=True)
    run_max = jnp.full((row_total,), -1e30, jnp.float32)
    scores = (
        jnp.einsum("rk,sk->rs", queries, key_part, preferred_element_type=jnp.float32)
        * softmax_scale
    )
    visible = key_pos[None, :] <= query_pos[:, None]
    new_max = jnp.maximum(run_max, jnp.max(jnp.where(visible, scores, -1e30), axis=1))
    weights = jnp.where(visible, jnp.exp(scores - new_max[:, None]), 0.0)
    new_sum = jnp.sum(weights, axis=1)
    added = jnp.dot(
        weights.astype(jnp.bfloat16), key_part[:, :latent], preferred_element_type=jnp.float32
    )
    o_lat = (added / new_sum[:, None]).astype(jnp.bfloat16).reshape(tok_count, head_count, latent)
    head_out = jnp.einsum("thl,hlv->thv", o_lat, up_value, preferred_element_type=jnp.float32)
    rows_out = head_out.astype(jnp.bfloat16).reshape(tok_count, -1)
    partial_value = jnp.dot(
        lax.all_gather(rows_out, "ctx", axis=0, tiled=True),
        w_out,
        preferred_element_type=jnp.float32,
    )
    summed = lax.psum_scatter(
        partial_value.astype(jnp.bfloat16), "tp", scatter_dimension=0, tiled=True
    )
    return summed


CHUNK_HEADS = 2
WINDOW = 2
EARLY = 1


def on_device(sizes, *args):
    q_nope, q_rope, c_kv, k_rope, positions, w_uk, w_uv, w_out = args
    n, groups, tps = sizes["ctx"], sizes["groups"], sizes["tp"]
    heads = w_uk.shape[0]
    chunks = heads // CHUNK_HEADS
    ends = 3 * chunks // 16
    mids = chunks // 2 - ends
    sz = dict(n=n, g=groups, t=tps, hc=CHUNK_HEADS, ends=ends, mids=mids, tok=q_nope.shape[0],
              window=WINDOW, early=EARLY,
              nope=w_uk.shape[1] * n, rope=k_rope.shape[1], lat=c_kv.shape[1],
              vdim=w_uv.shape[2], tile=w_out.shape[1] // 2)
    seq = n * sz["tok"]
    cols = w_out.shape[1]
    fits = (
        n == 4
        and tps == 4
        and heads % (2 * CHUNK_HEADS) == 0
        and CHUNK_HEADS % groups == 0
        and mids >= ends > EARLY + 1
        and seq <= 512
        and seq % (tps * 16) == 0
        and sz["tok"] % (tps * 16) == 0
        and sz["rope"] == 64
        and sz["nope"] % 128 == 0
        and sz["vdim"] % 128 == 0
        and sz["lat"] % 128 == 0
        and cols % 256 == 0
        and w_out.size * 2 + seq * cols * 8 <= 32 * 2**20
    )
    if fits:
        return fast(sz, *args)
    return general(*args)


def solution(mesh):
    in_specs = (
        P(("groups", "ctx"), "tp"),
        P(("groups", "ctx"), "tp"),
        P(("groups", "ctx"), None),
        P(("groups", "ctx"), None),
        P(("groups", "ctx")),
        P("tp", "ctx", None),
        P("tp", "ctx", None),
        P("tp", "ctx"),
    )
    out_specs = P(("groups", "tp"), "ctx")
    return jax.shard_map(
        functools.partial(on_device, dict(mesh.shape)),
        mesh=mesh, in_specs=in_specs, out_specs=out_specs, check_vma=False,
    )
```

```python
import functools
import math

import jax
import jax.numpy as jnp
from jax import lax
from jax.experimental import pallas as pl
from jax.experimental.pallas import tpu as pltpu
from jax.sharding import PartitionSpec as P

F32 = jnp.float32
BF16 = jnp.bfloat16
MESH = pl.DeviceIdType.MESH


def rotate(values, position):
    half_dim = values.shape[-1] // 2
    freqs = 10000.0 ** (-jnp.arange(half_dim, dtype=jnp.float32) / half_dim)
    angles = position.astype(jnp.float32)[..., None] * freqs
    cosine = jnp.cos(angles)
    sine = jnp.sin(angles)
    first_half = values[..., :half_dim].astype(jnp.float32)
    second_half = values[..., half_dim:].astype(jnp.float32)
    return jnp.concatenate(
        [first_half * cosine - second_half * sine, second_half * cosine + first_half * sine],
        axis=-1,
    )


def mega(sz, qn_in, qr_in, kv_in, kr_in, pos_in, wuk_in, wuv_in, wout_in, out_ref,
         qn, qr, kv, kr, pos, wuk, wuv, wout, krot, table, limit, ho, acc, part, got,
         s_w, s_q, s_k, r_w, r_q, r_k, r_p, s_y, r_y, s_t, r_t, s_ag, r_ag, s_rs, r_rs, loc_out):
    n, groups, tps, ends, mids = sz["n"], sz["g"], sz["t"], sz["ends"], sz["mids"]
    tok, hc, nope, rope, lat, vdim = (sz[k] for k in ("tok", "hc", "nope", "rope", "lat", "vdim"))
    scale = (nope + rope) ** (-0.5)
    hg = hc // groups
    c = lax.axis_index("ctx")
    g = lax.axis_index("groups")
    t = lax.axis_index("tp")
    nsl = nope // n
    lsl = lat // n
    share = tok // tps
    seq = n * tok

    def outer(j):
        return jnp.logical_or(j == 0, j == n - 1)

    def count(j):
        return jnp.where(outer(j), ends, mids)

    def begin(j):
        return jnp.where(j == 0, 0, ends + (j - 1) * mids)

    mine = count(c)
    first_mine = begin(c)
    at_end = outer(c)

    barrier = pltpu.get_barrier_semaphore()
    for axis, me, size in (("ctx", c, n), ("groups", g, groups), ("tp", t, tps)):
        for d in range(1, size):
            pl.semaphore_signal(barrier, inc=1, device_id={axis: lax.rem(me + d, size)}, device_id_type=MESH)
    pl.semaphore_wait(barrier, (n - 1) + (groups - 1) + (tps - 1))

    def al(x, m):
        return pl.multiple_of(x, m)

    def guard(i, j, body):
        if i < ends:
            body()
        else:
            pl.when(jnp.logical_not(outer(j)))(body)

    def rows_of(s):
        return pl.ds(al(s * tok, tok), tok)

    def piece(kind, i, j, s, part_of):
        if kind in (0, 5):
            src, dst = (kv_in, kv) if kind == 0 else (kr_in, kr)
            if part_of is None:
                return src, dst.at[rows_of(s), :]
            return (src.at[pl.ds(al(part_of * share, share), share), :],
                    dst.at[pl.ds(al(s * tok + part_of * share, share), share), :])
        if kind == 6:
            return pos_in, pos.at[s]
        if kind == 1:
            w = hc * nope
            return (qn_in.at[:, pl.ds(al((begin(j) + i) * w, w), w)],
                    qn.at[rows_of(s), pl.ds(i * w, w)])
        if kind == 2:
            w = hc * rope
            return (qr_in.at[:, pl.ds(al((begin(j) + i) * w, w), w)],
                    qr.at[rows_of(s), pl.ds(i * w, w)])
        if part_of is None:
            src_h, dst_h = pl.ds((begin(j) + i) * hc, hc), pl.ds(i * hc, hc)
        else:
            src_h = pl.ds((begin(j) + i) * hc + part_of * hg, hg)
            dst_h = pl.ds(i * hc + part_of * hg, hg)
        if kind == 3:
            return wuk_in.at[src_h], wuk.at[dst_h, pl.ds(al(s * nsl, nsl), nsl), :]
        return wuv_in.at[src_h], wuv.at[dst_h, pl.ds(al(s * lsl, lsl), lsl), :]

    def copy1(kind, i, d, sending):
        owner = t if kind in (0, 5) else g
        if sending:
            j = lax.rem(c + d, n)
            src, dst = piece(kind, i, j, c, owner)
        else:
            j = lax.rem(c + n - d, n)
            src, dst = piece(kind, i, c, j, owner)
        if kind in (3, 4):
            send, recv = s_w.at[i], r_w.at[i, d - 1]
        elif kind in (1, 2):
            send, recv = s_q.at[i], r_q.at[i]
        elif kind == 6:
            send, recv = s_k.at[2], r_p
        else:
            send, recv = s_k.at[kind // 5], r_k.at[kind // 5, d - 1]
        return pltpu.make_async_remote_copy(
            src_ref=src, dst_ref=dst, send_sem=send, recv_sem=recv,
            device_id={"ctx": j}, device_id_type=MESH)

    def local(kind, i):
        src, dst = piece(kind, i, c, c, None)
        if kind in (3, 4):
            sem = r_y.at[i]
        elif kind in (1, 2):
            sem = r_q.at[i]
        else:
            sem = r_p if kind == 6 else r_t.at[kind // 5]
        return pltpu.make_async_copy(src, dst, sem)

    def take(ref, sem):
        pltpu.make_async_copy(ref, ref, sem).wait()

    def weight_bytes(blocks):
        return wuk.at[pl.ds(0, blocks), pl.ds(0, nsl), :]

    def query_bytes(blocks):
        return qn.at[pl.ds(0, blocks * tok), pl.ds(0, hc * (nope + rope))]

    def key_bytes(kind, rows):
        return (kr if kind else kv).at[pl.ds(0, rows), :]

    def kinds(i):
        return (0, 1, 2, 3, 4, 5, 6) if i == 0 else (1, 2, 3, 4)

    def issue(i, group):
        for d in range(n - 1, 0, -1):
            def go():
                for kind in group:
                    copy1(kind, i, d, True).start()
            guard(i, lax.rem(c + d, n), go)

    def issue_chunk(i):
        issue(i, (3, 4))
        issue(i, (1, 2))

    issue(0, (6, 0, 5))
    window = sz["window"]
    for i in range(mids):
        if i < window:
            issue_chunk(i)
        else:
            pl.when(at_end)(functools.partial(issue_chunk, i))
    for i in range(mids):
        def go():
            for kind in kinds(i):
                local(kind, i).start()
        guard(i, c, go)
    wout_copy = pltpu.make_async_copy(wout_in, wout, loc_out)
    wout_copy.start()

    def copy_y(kind, i, e, d, sending):
        s = lax.rem(c + n - d, n)
        owner = g if sending else lax.rem(g + groups - e, groups)
        _, dst = piece(kind, i, c, s, owner)
        to = lax.rem(g + e, groups) if sending else owner
        return pltpu.make_async_remote_copy(
            src_ref=dst, dst_ref=dst, send_sem=s_y.at[i], recv_sem=r_y.at[i],
            device_id={"groups": to}, device_id_type=MESH)

    def copy_t(kind, e, d, sending):
        s = lax.rem(c + n - d, n)
        owner = t if sending else lax.rem(t + tps - e, tps)
        _, dst = piece(kind, 0, c, s, owner)
        to = lax.rem(t + e, tps) if sending else owner
        return pltpu.make_async_remote_copy(
            src_ref=dst, dst_ref=dst, send_sem=s_t.at[kind // 5], recv_sem=r_t.at[kind // 5],
            device_id={"tp": to}, device_id_type=MESH)

    def forward_weights(i):
        for d in range(n - 1, 0, -1):
            take(weight_bytes(2 * hg), r_w.at[i, d - 1])
            for kind in (3, 4):
                for e in range(1, groups):
                    copy_y(kind, i, e, d, True).start()

    def forward_keys():
        for d in range(1, n):
            for kind in (0, 5):
                copy1(kind, 0, d, False).wait_recv()
                for e in range(1, tps):
                    copy_t(kind, e, d, True).start()

    wide = 2 * rope

    def turn(x):
        lane = lax.broadcasted_iota(jnp.int32, x.shape, 1)
        low = lax.rem(lane, rope) < rope // 2
        other = jnp.where(low, -pltpu.roll(x, wide - rope // 2, 1), pltpu.roll(x, rope // 2, 1))
        return x * table[0] + other * table[1]

    def tables():
        take(pos, r_p)
        row = jnp.concatenate([pos[s] for s in range(n)], axis=1).astype(F32)
        col = jnp.broadcast_to(row, (wide, seq)).T
        lane = lax.broadcasted_iota(jnp.int32, (1, wide), 1)
        index = lax.rem(lane, rope // 2).astype(F32)
        freqs = jnp.exp(index * (-math.log(10000.0) / (rope // 2)))
        angles = col * freqs
        table[0] = jnp.cos(angles)
        table[1] = jnp.sin(angles)
        limit[...] = jnp.where(row > col[:, :1], -1e30, 3e38)

    def keys():
        for kind in (0, 5):
            take(key_bytes(kind, tok + (n - 1) * (tps - 1) * share), r_t.at[kind // 5])
        raw = kr[...].astype(F32)
        turned = turn(jnp.concatenate([raw, raw], axis=1))
        lane = lax.broadcasted_iota(jnp.int32, turned.shape, 1)
        krot[0] = jnp.where(lane < rope, turned, 0.0).astype(BF16)
        krot[1] = jnp.where(lane < rope, 0.0, turned).astype(BF16)

    def attend(i):
        nt = (((1,), (1,)), ((), ()))

        def pair(p, carry):
            raw = qr[:, pl.ds(al((i * (hc // 2) + p) * wide, wide), wide)]
            qrp = turn(raw.astype(F32)).astype(BF16)
            for k in range(2):
                hl = 2 * p + k
                h = i * hc + hl
                q = qn[:, pl.ds(al(h * nope, nope), nope)]
                ql = jnp.dot(q, wuk[h], preferred_element_type=F32).astype(BF16)
                sc = lax.dot_general(ql, kv[...], nt, preferred_element_type=F32)
                sc = (sc + lax.dot_general(qrp, krot[k], nt, preferred_element_type=F32)) * scale
                sc = jnp.minimum(sc, limit[...])
                w = jnp.exp(sc - jnp.max(sc, axis=1, keepdims=True))
                total = jnp.sum(w, axis=1, keepdims=True)
                o = jnp.dot(w.astype(BF16), kv[...], preferred_element_type=F32)
                o = (o / total).astype(BF16)
                ho[first_mine + i, :, pl.ds(al(hl * vdim, vdim), vdim)] = jnp.dot(
                    o, wuv[h], preferred_element_type=F32).astype(BF16)
            return carry

        lax.fori_loop(0, hc // 2, pair, 0)

    away, stay = 0, 1
    half_rows = seq // 2
    side = t // 2

    def rows_half(h):
        return pl.ds(al((1 - side if h == away else side) * half_rows, half_rows), half_rows)

    def ag_copy(q, h, right):
        ref = ho.at[q, rows_half(h), :]
        return pltpu.make_async_remote_copy(
            src_ref=ref, dst_ref=ref, send_sem=s_ag.at[1 if right else 0],
            recv_sem=r_ag.at[q, h],
            device_id={"ctx": c + 1 if right else c - 1}, device_id_type=MESH)

    inner_right = c < n // 2

    def send_inward(i, h):
        pl.when(inner_right)(lambda: ag_copy(first_mine + i, h, True).start())
        pl.when(jnp.logical_not(inner_right))(lambda: ag_copy(first_mine + i, h, False).start())

    def send_outward(i, h):
        pl.when(jnp.logical_and(inner_right, c > 0))(
            lambda: ag_copy(first_mine + i, h, False).start())
        pl.when(jnp.logical_and(jnp.logical_not(inner_right), c + 1 < n))(
            lambda: ag_copy(first_mine + i, h, True).start())

    cols = acc.shape[1]
    tile = sz["tile"]
    kdim = hc * vdim

    def project(q, rows, first=False):
        depth = pl.ds(al(q * kdim, kdim), kdim)

        def step(j, carry):
            at = pl.ds(al(j * tile, tile), tile)
            value = jnp.dot(ho[q, rows, :], wout[depth, at], preferred_element_type=F32)
            acc[rows, at] = value if first else acc[rows, at] + value
            return carry

        lax.fori_loop(0, cols // tile, step, 0)

    def handle(d, i, h):
        @pl.when(jnp.logical_and(c + d < n, i < count(c + d)))
        def _():
            q = begin(c + d) + i
            ag_copy(q, h, False).wait_recv()
            pl.when(c > 0)(lambda: ag_copy(q, h, False).start())
            project(q, rows_half(h))

        @pl.when(jnp.logical_and(c - d >= 0, i < count(c - d)))
        def _():
            q = begin(c - d) + i
            ag_copy(q, h, True).wait_recv()
            pl.when(c + 1 < n)(lambda: ag_copy(q, h, True).start())
            project(q, rows_half(h))

    def handle_all(d, low, high, h):
        def body(i, carry):
            handle(d, i, h)
            return carry

        lax.fori_loop(low, high, body, 0)

    early = sz["early"]

    def chunk(i):
        take(query_bytes(n), r_q.at[i])
        take(weight_bytes((n - 1) * (groups - 1) * 2 * hg + 2 * hc), r_y.at[i])
        attend(i)
        if i + window < mids:
            pl.when(jnp.logical_not(at_end))(functools.partial(issue_chunk, i + window))
        send_outward(i, away)
        send_inward(i, away)
        send_outward(i, stay)
        if i < early:
            send_inward(i, stay)
        if i == 0:
            wout_copy.wait()
        project(first_mine + i, slice(None), i == 0)
        if i > 0:
            handle(1, i - 1, away)
            if i - 1 < early:
                handle(1, i - 1, stay)

    forward_keys()
    forward_weights(0)
    tables()
    keys()
    guard(0, c, functools.partial(chunk, 0))
    for i in range(1, mids):
        guard(i, c, functools.partial(forward_weights, i))
        guard(i, c, functools.partial(chunk, i))

    def send_late():
        for i in range(early, mids):
            guard(i, c, functools.partial(send_inward, i, stay))

    pl.when(at_end)(send_late)
    handle_all(1, mine - 1, mids, away)
    pl.when(jnp.logical_not(at_end))(send_late)

    rows_out = out_ref.shape[0]
    half = cols // 2
    core = lax.rem(t, 2)
    mate = t + 1 - 2 * core
    across = lax.rem(t + 2, tps)
    mate_across = lax.rem(mate + 2, tps)

    def block(r, at):
        return acc[pl.ds(al(r * rows_out, rows_out), rows_out), at]

    def rs_copy(stage, k):
        at = pl.ds(k * half, half)
        slot = (1, 2, 0)[stage]
        return pltpu.make_async_remote_copy(
            src_ref=part.at[slot, :, at], dst_ref=got.at[slot, :, at],
            send_sem=s_rs, recv_sem=r_rs.at[stage, k],
            device_id={"tp": across if stage == 1 else mate}, device_id_type=MESH)

    spans = [slice(k * half, (k + 1) * half) for k in range(2)]

    handle_all(2, 0, mids, away)
    for i in range(mids):
        guard(i, c, lambda: take(weight_bytes((n - 1) * (groups - 1) * 2 * hg), s_y.at[i]))
    handle_all(3, 0, ends, away)
    for k, at in enumerate(spans):
        part[1, :, at] = block(mate_across, at).astype(BF16)
        rs_copy(0, k).start()
    handle(1, early, stay)
    for k, at in enumerate(spans):
        rs_copy(0, k).wait_recv()
        part[2, :, at] = (block(across, at) + got[1, :, at].astype(F32)).astype(BF16)
        rs_copy(1, k).start()
    handle_all(1, early + 1, mids, stay)
    def sent(i, peers):
        take(weight_bytes(peers * 2 * hg), s_w.at[i])
        take(query_bytes(peers), s_q.at[i])

    for i in range(mids):
        if i < ends:
            sent(i, n - 1)
        else:
            pl.when(at_end)(functools.partial(sent, i, n - 2))
            pl.when(jnp.logical_not(at_end))(functools.partial(sent, i, n - 3))
    for kind in (0, 5):
        take(key_bytes(kind, (n - 1) * share), s_k.at[kind // 5])
        take(key_bytes(kind, (n - 1) * (tps - 1) * share), s_t.at[kind // 5])
    take(pos.at[pl.ds(0, n - 1)], s_k.at[2])
    handle_all(2, 0, mids, stay)

    def drain():
        for b in range(n):
            low = 0 if b == 0 else ends + (b - 1) * mids
            high = low + (ends if b in (0, n - 1) else mids)

            @pl.when(c == b)
            def _():
                if b + 1 < n:
                    take(ho.at[pl.ds(0, high)], s_ag.at[1])
                if b > 0:
                    take(ho.at[pl.ds(low, ho.shape[0] - low)], s_ag.at[0])

    handle_all(3, 0, ends, stay)
    for k, at in enumerate(spans):
        part[0, :, at] = block(mate, at).astype(BF16)
        rs_copy(2, k).start()
    for k, at in enumerate(spans):
        rs_copy(1, k).wait_recv()
        own = block(t, at) + got[2, :, at].astype(F32)
        rs_copy(2, k).wait_recv()
        out_ref[:, at] = (own + got[0, :, at].astype(F32)).astype(BF16)
    take(part, s_rs)
    drain()


def fast(sz, q_nope, q_rope, c_kv, k_rope, positions, w_uk, w_uv, w_out):
    n, groups, tps, ends, mids = sz["n"], sz["g"], sz["t"], sz["ends"], sz["mids"]
    tok, hc, nope, rope, lat, vdim = (sz[k] for k in ("tok", "hc", "nope", "rope", "lat", "vdim"))
    heads = w_uk.shape[0]
    chunks = heads // hc
    hpc = mids * hc
    seq = n * tok
    cols = w_out.shape[1]
    hbm = pl.BlockSpec(memory_space=pltpu.HBM)
    dma = pltpu.SemaphoreType.DMA
    return pl.pallas_call(
        functools.partial(mega, sz),
        out_shape=jax.ShapeDtypeStruct((seq // tps, cols), BF16),
        in_specs=[hbm] * 8,
        out_specs=pl.BlockSpec(memory_space=pltpu.VMEM),
        scratch_shapes=[
            pltpu.VMEM((seq, hpc * nope), BF16),
            pltpu.VMEM((seq, hpc * rope), BF16),
            pltpu.VMEM((seq, lat), BF16),
            pltpu.VMEM((seq, rope), BF16),
            pltpu.VMEM((n, 1, tok), jnp.int32),
            pltpu.VMEM((hpc, nope, lat), BF16),
            pltpu.VMEM((hpc, lat, vdim), BF16),
            pltpu.VMEM(w_out.shape, BF16),
            pltpu.VMEM((2, seq, 2 * rope), BF16),
            pltpu.VMEM((2, seq, 2 * rope), F32),
            pltpu.VMEM((seq, seq), F32),
            pltpu.VMEM((chunks, seq, hc * vdim), BF16),
            pltpu.VMEM((seq, cols), F32),
            pltpu.VMEM((tps - 1, seq // tps, cols), BF16),
            pltpu.VMEM((tps - 1, seq // tps, cols), BF16),
            dma((mids,)),
            dma((mids,)),
            dma((3,)),
            dma((mids, n - 1)),
            dma((mids,)),
            dma((2, n - 1)),
            dma,
            dma((mids,)),
            dma((mids,)),
            dma((2,)),
            dma((2,)),
            dma((2,)),
            dma((chunks, 2)),
            dma,
            dma((3, 2)),
            dma,
        ],
        compiler_params=pltpu.CompilerParams(collective_id=0, has_side_effects=True,
                                             vmem_limit_bytes=60 * 1024 * 1024),
    )(q_nope, q_rope, c_kv, k_rope, positions.reshape(1, tok), w_uk, w_uv, w_out)


def general(q_nope, q_rope, c_kv, k_rope, positions, w_uk, w_uv, w_out):
    tok_count = q_nope.shape[0]
    head_count = w_uk.shape[0]
    latent = c_kv.shape[1]
    up_key, up_value = (
        lax.all_gather(w_uk, "ctx", axis=1, tiled=True),
        lax.all_gather(w_uv, "ctx", axis=1, tiled=True),
    )
    nope_dim = up_key.shape[1]
    rope_dim = k_rope.shape[1]
    softmax_scale = (nope_dim + rope_dim) ** (-0.5)
    q_parts = q_nope.reshape(tok_count, head_count, nope_dim)
    q_lat = jnp.einsum("thn,hnl->thl", q_parts, up_key, preferred_element_type=jnp.float32).astype(
        jnp.bfloat16
    )
    q_rot = rotate(q_rope.reshape(tok_count, head_count, rope_dim), positions[:, None]).astype(
        jnp.bfloat16
    )
    k_rot = rotate(k_rope, positions).astype(jnp.bfloat16)
    key_rows = jnp.concatenate([c_kv, k_rot], axis=1)
    queries = jnp.concatenate([q_lat, q_rot], axis=2).reshape(
        tok_count * head_count, latent + rope_dim
    )
    query_pos = jnp.repeat(positions, head_count)
    row_total = tok_count * head_count
    key_part = lax.all_gather(key_rows, "ctx", axis=0, tiled=True)
    key_pos = lax.all_gather(positions, "ctx", axis=0, tiled=True)
    run_max = jnp.full((row_total,), -1e30, jnp.float32)
    scores = (
        jnp.einsum("rk,sk->rs", queries, key_part, preferred_element_type=jnp.float32)
        * softmax_scale
    )
    visible = key_pos[None, :] <= query_pos[:, None]
    new_max = jnp.maximum(run_max, jnp.max(jnp.where(visible, scores, -1e30), axis=1))
    weights = jnp.where(visible, jnp.exp(scores - new_max[:, None]), 0.0)
    new_sum = jnp.sum(weights, axis=1)
    added = jnp.dot(
        weights.astype(jnp.bfloat16), key_part[:, :latent], preferred_element_type=jnp.float32
    )
    o_lat = (added / new_sum[:, None]).astype(jnp.bfloat16).reshape(tok_count, head_count, latent)
    head_out = jnp.einsum("thl,hlv->thv", o_lat, up_value, preferred_element_type=jnp.float32)
    rows_out = head_out.astype(jnp.bfloat16).reshape(tok_count, -1)
    partial_value = jnp.dot(
        lax.all_gather(rows_out, "ctx", axis=0, tiled=True),
        w_out,
        preferred_element_type=jnp.float32,
    )
    summed = lax.psum_scatter(
        partial_value.astype(jnp.bfloat16), "tp", scatter_dimension=0, tiled=True
    )
    return summed


CHUNK_HEADS = 2
WINDOW = 2
EARLY = 1


def on_device(sizes, *args):
    q_nope, q_rope, c_kv, k_rope, positions, w_uk, w_uv, w_out = args
    n, groups, tps = sizes["ctx"], sizes["groups"], sizes["tp"]
    heads = w_uk.shape[0]
    chunks = heads // CHUNK_HEADS
    ends = 3 * chunks // 16
    mids = chunks // 2 - ends
    sz = dict(n=n, g=groups, t=tps, hc=CHUNK_HEADS, ends=ends, mids=mids, tok=q_nope.shape[0],
              window=WINDOW, early=EARLY,
              nope=w_uk.shape[1] * n, rope=k_rope.shape[1], lat=c_kv.shape[1],
              vdim=w_uv.shape[2], tile=w_out.shape[1] // 2)
    seq = n * sz["tok"]
    cols = w_out.shape[1]
    fits = (
        n == 4
        and tps == 4
        and heads % (2 * CHUNK_HEADS) == 0
        and CHUNK_HEADS % groups == 0
        and groups == 2
        and mids >= ends > EARLY + 1
        and mids >= n + 1
        and sz["nope"] == sz["vdim"]
        and seq <= 512
        and seq % (tps * 16) == 0
        and sz["tok"] % (tps * 16) == 0
        and sz["rope"] == 64
        and sz["nope"] % 128 == 0
        and sz["vdim"] % 128 == 0
        and sz["lat"] % 128 == 0
        and cols % 256 == 0
        and w_out.size * 2 + seq * cols * 8 <= 32 * 2**20
    )
    if fits:
        return fast(sz, *args)
    return general(*args)


def solution(mesh):
    in_specs = (
        P(("groups", "ctx"), "tp"),
        P(("groups", "ctx"), "tp"),
        P(("groups", "ctx"), None),
        P(("groups", "ctx"), None),
        P(("groups", "ctx")),
        P("tp", "ctx", None),
        P("tp", "ctx", None),
        P("tp", "ctx"),
    )
    out_specs = P(("groups", "tp"), "ctx")
    return jax.shard_map(
        functools.partial(on_device, dict(mesh.shape)),
        mesh=mesh, in_specs=in_specs, out_specs=out_specs, check_vma=False,
    )
```

```python
import functools
import math

import jax
import jax.numpy as jnp
from jax import lax
from jax.experimental import pallas as pl
from jax.experimental.pallas import tpu as pltpu
from jax.sharding import PartitionSpec as P

F32 = jnp.float32
BF16 = jnp.bfloat16
MESH = pl.DeviceIdType.MESH


def rotate(values, position):
    half_dim = values.shape[-1] // 2
    freqs = 10000.0 ** (-jnp.arange(half_dim, dtype=jnp.float32) / half_dim)
    angles = position.astype(jnp.float32)[..., None] * freqs
    cosine = jnp.cos(angles)
    sine = jnp.sin(angles)
    first_half = values[..., :half_dim].astype(jnp.float32)
    second_half = values[..., half_dim:].astype(jnp.float32)
    return jnp.concatenate(
        [first_half * cosine - second_half * sine, second_half * cosine + first_half * sine],
        axis=-1,
    )


def mega(sz, qn_in, qr_in, kv_in, kr_in, pos_in, wuk_in, wuv_in, wout_in, out_ref,
         qn, qr, kv, kr, pos, wuk, wuv, wout, krot, table, limit, ho, acc, part, got,
         s_w, s_q, s_k, r_w, r_q, r_k, r_p, s_y, r_y, s_t, r_t, s_ag, r_ag, s_rs, r_rs, loc_out):
    n, groups, tps, ends, mids = sz["n"], sz["g"], sz["t"], sz["ends"], sz["mids"]
    tok, hc, nope, rope, lat, vdim = (sz[k] for k in ("tok", "hc", "nope", "rope", "lat", "vdim"))
    scale = (nope + rope) ** (-0.5)
    hg = hc // groups
    c = lax.axis_index("ctx")
    g = lax.axis_index("groups")
    t = lax.axis_index("tp")
    nsl = nope // n
    lsl = lat // n
    share = tok // tps
    seq = n * tok

    def outer(j):
        return jnp.logical_or(j == 0, j == n - 1)

    def count(j):
        return jnp.where(outer(j), ends, mids)

    def begin(j):
        return jnp.where(j == 0, 0, ends + (j - 1) * mids)

    mine = count(c)
    first_mine = begin(c)
    at_end = outer(c)

    barrier = pltpu.get_barrier_semaphore()
    for axis, me, size in (("ctx", c, n), ("groups", g, groups), ("tp", t, tps)):
        for d in range(1, size):
            pl.semaphore_signal(barrier, inc=1, device_id={axis: lax.rem(me + d, size)}, device_id_type=MESH)
    pl.semaphore_wait(barrier, (n - 1) + (groups - 1) + (tps - 1))

    def al(x, m):
        return pl.multiple_of(x, m)

    def guard(i, j, body):
        if i < ends:
            body()
        else:
            pl.when(jnp.logical_not(outer(j)))(body)

    def rows_of(s):
        return pl.ds(al(s * tok, tok), tok)

    def piece(kind, i, j, s, part_of):
        if kind in (0, 5):
            src, dst = (kv_in, kv) if kind == 0 else (kr_in, kr)
            if part_of is None:
                return src, dst.at[rows_of(s), :]
            return (src.at[pl.ds(al(part_of * share, share), share), :],
                    dst.at[pl.ds(al(s * tok + part_of * share, share), share), :])
        if kind == 6:
            return pos_in, pos.at[s]
        if kind == 1:
            w = hc * nope
            return (qn_in.at[:, pl.ds(al((begin(j) + i) * w, w), w)],
                    qn.at[rows_of(s), pl.ds(i * w, w)])
        if kind == 2:
            w = hc * rope
            return (qr_in.at[:, pl.ds(al((begin(j) + i) * w, w), w)],
                    qr.at[rows_of(s), pl.ds(i * w, w)])
        if part_of is None:
            src_h, dst_h = pl.ds((begin(j) + i) * hc, hc), pl.ds(i * hc, hc)
        else:
            src_h = pl.ds((begin(j) + i) * hc + part_of * hg, hg)
            dst_h = pl.ds(i * hc + part_of * hg, hg)
        if kind == 3:
            return wuk_in.at[src_h], wuk.at[dst_h, pl.ds(al(s * nsl, nsl), nsl), :]
        return wuv_in.at[src_h], wuv.at[dst_h, pl.ds(al(s * lsl, lsl), lsl), :]

    def copy1(kind, i, d, to=None):
        owner = t if kind in (0, 5) else g
        if to is not None:
            j = to
            src, dst = piece(kind, i, j, c, owner)
        else:
            j = lax.rem(c + n - d, n)
            src, dst = piece(kind, i, c, j, owner)
        if kind in (3, 4):
            send, recv = s_w.at[i], r_w.at[i, d - 1]
        elif kind in (1, 2):
            send, recv = s_q.at[i], r_q.at[i]
        elif kind == 6:
            send, recv = s_k.at[2], r_p
        else:
            send, recv = s_k.at[kind // 5], r_k.at[kind // 5, d - 1]
        return pltpu.make_async_remote_copy(
            src_ref=src, dst_ref=dst, send_sem=send, recv_sem=recv,
            device_id={"ctx": j}, device_id_type=MESH)

    def local(kind, i):
        src, dst = piece(kind, i, c, c, None)
        if kind in (3, 4):
            sem = r_y.at[i]
        elif kind in (1, 2):
            sem = r_q.at[i]
        else:
            sem = r_p if kind == 6 else r_t.at[kind // 5]
        return pltpu.make_async_copy(src, dst, sem)

    def take(ref, sem):
        pltpu.make_async_copy(ref, ref, sem).wait()

    def weight_bytes(blocks):
        return wuk.at[pl.ds(0, blocks), pl.ds(0, nsl), :]

    def query_bytes(blocks):
        return qn.at[pl.ds(0, blocks * tok), pl.ds(0, hc * (nope + rope))]

    def key_bytes(kind, rows):
        return (kr if kind else kv).at[pl.ds(0, rows), :]

    def kinds(i):
        return (0, 1, 2, 3, 4, 5, 6) if i == 0 else (1, 2, 3, 4)

    def turns(total):
        order = [((3, 4), 0)]
        for i in range(total):
            if i + 1 < total:
                order.append(((3, 4), i + 1))
            order.append(((1, 2), i))
        return order

    def send_chunks(b, total, targets):
        for group, i in turns(total):
            for j in targets:
                for kind in group:
                    copy1(kind, i, (j - b) % n, j).start()

    sides = (0, n - 1)

    def far_ends(b):
        if b in sides:
            return [n - 1 - b]
        return [0 if b >= n // 2 else n - 1]

    for b in range(n):
        @pl.when(c == b)
        def _():
            by_distance = sorted((j for j in range(n) if j != b), key=lambda j: -abs(j - b))
            for kind in (6, 0, 5):
                for j in by_distance:
                    copy1(kind, 0, (j - b) % n, j).start()
            if b not in sides:
                send_chunks(b, ends, [n - 1 - far_ends(b)[0]])
            send_chunks(b, mids, [j for j in by_distance if j not in sides])
            if b in sides or sz["release"] < 0:
                send_chunks(b, ends, far_ends(b))

    def send_far():
        for b in range(1, n - 1):
            pl.when(c == b)(functools.partial(send_chunks, b, ends, far_ends(b)))

    for i in range(mids):
        def go():
            for kind in kinds(i):
                local(kind, i).start()
        guard(i, c, go)
    wout_copy = pltpu.make_async_copy(wout_in, wout, loc_out)
    wout_copy.start()

    def copy_y(kind, i, e, d, sending):
        s = lax.rem(c + n - d, n)
        owner = g if sending else lax.rem(g + groups - e, groups)
        _, dst = piece(kind, i, c, s, owner)
        to = lax.rem(g + e, groups) if sending else owner
        return pltpu.make_async_remote_copy(
            src_ref=dst, dst_ref=dst, send_sem=s_y.at[i], recv_sem=r_y.at[i],
            device_id={"groups": to}, device_id_type=MESH)

    def copy_t(kind, e, d, sending):
        s = lax.rem(c + n - d, n)
        owner = t if sending else lax.rem(t + tps - e, tps)
        _, dst = piece(kind, 0, c, s, owner)
        to = lax.rem(t + e, tps) if sending else owner
        return pltpu.make_async_remote_copy(
            src_ref=dst, dst_ref=dst, send_sem=s_t.at[kind // 5], recv_sem=r_t.at[kind // 5],
            device_id={"tp": to}, device_id_type=MESH)

    def forward_from(i, d):
        take(weight_bytes(2 * hg), r_w.at[i, d - 1])
        for kind in (3, 4):
            for e in range(1, groups):
                copy_y(kind, i, e, d, True).start()

    def forward_weights(i):
        @pl.when(jnp.logical_not(at_end))
        def _():
            forward_from(i, 3)
            forward_from(i, 1)

        forward_from(i, 2)

    def forward_others(near, far):
        for d in (near, far):
            for i in range(ends):
                forward_from(i, d)

    def forward_keys():
        for d in range(1, n):
            for kind in (0, 5):
                copy1(kind, 0, d).wait_recv()
                for e in range(1, tps):
                    copy_t(kind, e, d, True).start()

    wide = 2 * rope

    def turn(x):
        lane = lax.broadcasted_iota(jnp.int32, x.shape, 1)
        low = lax.rem(lane, rope) < rope // 2
        other = jnp.where(low, -pltpu.roll(x, wide - rope // 2, 1), pltpu.roll(x, rope // 2, 1))
        return x * table[0] + other * table[1]

    def tables():
        take(pos, r_p)
        row = jnp.concatenate([pos[s] for s in range(n)], axis=1).astype(F32)
        col = jnp.broadcast_to(row, (wide, seq)).T
        lane = lax.broadcasted_iota(jnp.int32, (1, wide), 1)
        index = lax.rem(lane, rope // 2).astype(F32)
        freqs = jnp.exp(index * (-math.log(10000.0) / (rope // 2)))
        angles = col * freqs
        table[0] = jnp.cos(angles)
        table[1] = jnp.sin(angles)
        limit[...] = jnp.where(row > col[:, :1], -1e30, 3e38)

    def keys():
        for kind in (0, 5):
            take(key_bytes(kind, tok + (n - 1) * (tps - 1) * share), r_t.at[kind // 5])
        raw = kr[...].astype(F32)
        turned = turn(jnp.concatenate([raw, raw], axis=1))
        lane = lax.broadcasted_iota(jnp.int32, turned.shape, 1)
        krot[0] = jnp.where(lane < rope, turned, 0.0).astype(BF16)
        krot[1] = jnp.where(lane < rope, 0.0, turned).astype(BF16)

    def attend(i):
        nt = (((1,), (1,)), ((), ()))

        def pair(p, carry):
            raw = qr[:, pl.ds(al((i * (hc // 2) + p) * wide, wide), wide)]
            qrp = turn(raw.astype(F32)).astype(BF16)
            for k in range(2):
                hl = 2 * p + k
                h = i * hc + hl
                q = qn[:, pl.ds(al(h * nope, nope), nope)]
                ql = jnp.dot(q, wuk[h], preferred_element_type=F32).astype(BF16)
                sc = lax.dot_general(ql, kv[...], nt, preferred_element_type=F32)
                sc = (sc + lax.dot_general(qrp, krot[k], nt, preferred_element_type=F32)) * scale
                sc = jnp.minimum(sc, limit[...])
                w = jnp.exp(sc - jnp.max(sc, axis=1, keepdims=True))
                total = jnp.sum(w, axis=1, keepdims=True)
                o = jnp.dot(w.astype(BF16), kv[...], preferred_element_type=F32)
                o = (o / total).astype(BF16)
                ho[first_mine + i, :, pl.ds(al(hl * vdim, vdim), vdim)] = jnp.dot(
                    o, wuv[h], preferred_element_type=F32).astype(BF16)
            return carry

        lax.fori_loop(0, hc // 2, pair, 0)

    away, stay = 0, 1
    half_rows = seq // 2
    side = t // 2

    def rows_half(h):
        return pl.ds(al((1 - side if h == away else side) * half_rows, half_rows), half_rows)

    def ag_copy(q, h, right):
        ref = ho.at[q, rows_half(h), :]
        return pltpu.make_async_remote_copy(
            src_ref=ref, dst_ref=ref, send_sem=s_ag.at[1 if right else 0],
            recv_sem=r_ag.at[q, h],
            device_id={"ctx": c + 1 if right else c - 1}, device_id_type=MESH)

    inner_right = c < n // 2

    def send_inward(i, h):
        pl.when(inner_right)(lambda: ag_copy(first_mine + i, h, True).start())
        pl.when(jnp.logical_not(inner_right))(lambda: ag_copy(first_mine + i, h, False).start())

    def send_outward(i, h):
        pl.when(jnp.logical_and(inner_right, c > 0))(
            lambda: ag_copy(first_mine + i, h, False).start())
        pl.when(jnp.logical_and(jnp.logical_not(inner_right), c + 1 < n))(
            lambda: ag_copy(first_mine + i, h, True).start())

    cols = acc.shape[1]
    tile = sz["tile"]
    kdim = hc * vdim

    def project(q, rows, first=False):
        depth = pl.ds(al(q * kdim, kdim), kdim)

        def step(j, carry):
            at = pl.ds(al(j * tile, tile), tile)
            value = jnp.dot(ho[q, rows, :], wout[depth, at], preferred_element_type=F32)
            acc[rows, at] = value if first else acc[rows, at] + value
            return carry

        lax.fori_loop(0, cols // tile, step, 0)

    def arrive(b, i, h, right):
        @pl.when(jnp.logical_and(jnp.logical_and(b >= 0, b < n), jnp.logical_and(i >= 0, i < count(b))))
        def _():
            q = begin(b) + i
            with jax.named_scope("take"):
                ag_copy(q, h, right).wait_recv()
            more = c + 1 < n if right else c > 0
            pl.when(more)(lambda: ag_copy(q, h, right).start())
            project(q, rows_half(h))

    def arrive_all(d, low, high, h):
        def body(i, carry):
            arrive(c + d, i, h, False)
            arrive(c - d, i, h, True)
            return carry

        lax.fori_loop(low, high, body, 0)

    def arrive_inward(i, h):
        pl.when(inner_right)(lambda: arrive(c + 1, i, h, False))
        pl.when(jnp.logical_not(inner_right))(lambda: arrive(c - 1, i, h, True))

    def arrive_outward(i, h):
        pl.when(inner_right)(lambda: arrive(c - 1, i, h, True))
        pl.when(jnp.logical_not(inner_right))(lambda: arrive(c + 1, i, h, False))

    early = sz["early"]

    def chunk(i):
        take(query_bytes(n), r_q.at[i])
        take(weight_bytes((n - 1) * (groups - 1) * 2 * hg + 2 * hc), r_y.at[i])
        attend(i)
        send_outward(i, away)
        send_inward(i, away)
        send_outward(i, stay)
        if i < early:
            pl.when(jnp.logical_not(at_end))(functools.partial(send_inward, i, stay))
        if i == sz["release"]:
            send_far()
        if i == 0:
            wout_copy.wait()
        project(first_mine + i, slice(None), i == 0)

    forward_keys()
    pl.when(c == 0)(functools.partial(forward_others, 3, 1))
    pl.when(c == n - 1)(functools.partial(forward_others, 1, 3))
    forward_weights(0)
    tables()
    keys()
    for i in range(mids):
        if i + 1 < mids:
            guard(i + 1, c, functools.partial(forward_weights, i + 1))
        guard(i, c, functools.partial(chunk, i))

    def send_late(low, high):
        for i in range(low, high):
            send_inward(i, stay)

    pl.when(at_end)(functools.partial(send_late, 0, ends))
    for i in range(early):
        arrive_inward(i, away)
        arrive_inward(i, stay)

    def first_away(i, carry):
        arrive_inward(i, away)
        arrive_outward(i - early - sz["behind"], away)
        return carry

    lax.fori_loop(early, ends + early + sz["behind"] + (mids - ends), first_away, 0)
    pl.when(jnp.logical_not(at_end))(functools.partial(send_late, early, mids))

    rows_out = out_ref.shape[0]
    half = cols // 2
    core = lax.rem(t, 2)
    mate = t + 1 - 2 * core
    across = lax.rem(t + 2, tps)
    mate_across = lax.rem(mate + 2, tps)

    def block(r, at):
        return acc[pl.ds(al(r * rows_out, rows_out), rows_out), at]

    def rs_copy(stage, k):
        at = pl.ds(k * half, half)
        slot = (1, 2, 0)[stage]
        return pltpu.make_async_remote_copy(
            src_ref=part.at[slot, :, at], dst_ref=got.at[slot, :, at],
            send_sem=s_rs, recv_sem=r_rs.at[stage, k],
            device_id={"tp": across if stage == 1 else mate}, device_id_type=MESH)

    spans = [slice(k * half, (k + 1) * half) for k in range(2)]

    arrive_all(2, 0, mids, away)
    for i in range(mids):
        guard(i, c, lambda: take(weight_bytes((n - 1) * (groups - 1) * 2 * hg), s_y.at[i]))
    arrive_all(3, 0, ends, away)
    for k, at in enumerate(spans):
        part[1, :, at] = block(mate_across, at).astype(BF16)
        rs_copy(0, k).start()
    arrive_inward(early, stay)
    arrive_outward(0, stay)
    for k, at in enumerate(spans):
        rs_copy(0, k).wait_recv()
        part[2, :, at] = (block(across, at) + got[1, :, at].astype(F32)).astype(BF16)
        rs_copy(1, k).start()

    def first_stay(i, carry):
        arrive_inward(i + early, stay)
        arrive_outward(i, stay)
        return carry

    lax.fori_loop(1, mids - early, first_stay, 0)
    def sent(i, peers):
        take(weight_bytes(peers * 2 * hg), s_w.at[i])
        take(query_bytes(peers), s_q.at[i])

    for i in range(mids):
        if i < ends:
            sent(i, n - 1)
        else:
            pl.when(at_end)(functools.partial(sent, i, n - 2))
            pl.when(jnp.logical_not(at_end))(functools.partial(sent, i, n - 3))
    for kind in (0, 5):
        take(key_bytes(kind, (n - 1) * share), s_k.at[kind // 5])
        take(key_bytes(kind, (n - 1) * (tps - 1) * share), s_t.at[kind // 5])
    take(pos.at[pl.ds(0, n - 1)], s_k.at[2])
    arrive_all(2, 0, mids, stay)

    def drain():
        for b in range(n):
            low = 0 if b == 0 else ends + (b - 1) * mids
            high = low + (ends if b in (0, n - 1) else mids)

            @pl.when(c == b)
            def _():
                if b + 1 < n:
                    take(ho.at[pl.ds(0, high)], s_ag.at[1])
                if b > 0:
                    take(ho.at[pl.ds(low, ho.shape[0] - low)], s_ag.at[0])

    arrive_all(3, 0, ends, stay)
    for k, at in enumerate(spans):
        part[0, :, at] = block(mate, at).astype(BF16)
        rs_copy(2, k).start()
    for k, at in enumerate(spans):
        rs_copy(1, k).wait_recv()
        own = block(t, at) + got[2, :, at].astype(F32)
        rs_copy(2, k).wait_recv()
        out_ref[:, at] = (own + got[0, :, at].astype(F32)).astype(BF16)
    take(part, s_rs)
    drain()


def fast(sz, q_nope, q_rope, c_kv, k_rope, positions, w_uk, w_uv, w_out):
    n, groups, tps, ends, mids = sz["n"], sz["g"], sz["t"], sz["ends"], sz["mids"]
    tok, hc, nope, rope, lat, vdim = (sz[k] for k in ("tok", "hc", "nope", "rope", "lat", "vdim"))
    heads = w_uk.shape[0]
    chunks = heads // hc
    hpc = mids * hc
    seq = n * tok
    cols = w_out.shape[1]
    hbm = pl.BlockSpec(memory_space=pltpu.HBM)
    dma = pltpu.SemaphoreType.DMA
    return pl.pallas_call(
        functools.partial(mega, sz),
        out_shape=jax.ShapeDtypeStruct((seq // tps, cols), BF16),
        in_specs=[hbm] * 8,
        out_specs=pl.BlockSpec(memory_space=pltpu.VMEM),
        scratch_shapes=[
            pltpu.VMEM((seq, hpc * nope), BF16),
            pltpu.VMEM((seq, hpc * rope), BF16),
            pltpu.VMEM((seq, lat), BF16),
            pltpu.VMEM((seq, rope), BF16),
            pltpu.VMEM((n, 1, tok), jnp.int32),
            pltpu.VMEM((hpc, nope, lat), BF16),
            pltpu.VMEM((hpc, lat, vdim), BF16),
            pltpu.VMEM(w_out.shape, BF16),
            pltpu.VMEM((2, seq, 2 * rope), BF16),
            pltpu.VMEM((2, seq, 2 * rope), F32),
            pltpu.VMEM((seq, seq), F32),
            pltpu.VMEM((chunks, seq, hc * vdim), BF16),
            pltpu.VMEM((seq, cols), F32),
            pltpu.VMEM((tps - 1, seq // tps, cols), BF16),
            pltpu.VMEM((tps - 1, seq // tps, cols), BF16),
            dma((mids,)),
            dma((mids,)),
            dma((3,)),
            dma((mids, n - 1)),
            dma((mids,)),
            dma((2, n - 1)),
            dma,
            dma((mids,)),
            dma((mids,)),
            dma((2,)),
            dma((2,)),
            dma((2,)),
            dma((chunks, 2)),
            dma,
            dma((3, 2)),
            dma,
        ],
        compiler_params=pltpu.CompilerParams(collective_id=0, has_side_effects=True,
                                             vmem_limit_bytes=60 * 1024 * 1024),
    )(q_nope, q_rope, c_kv, k_rope, positions.reshape(1, tok), w_uk, w_uv, w_out)


def general(q_nope, q_rope, c_kv, k_rope, positions, w_uk, w_uv, w_out):
    tok_count = q_nope.shape[0]
    head_count = w_uk.shape[0]
    latent = c_kv.shape[1]
    up_key, up_value = (
        lax.all_gather(w_uk, "ctx", axis=1, tiled=True),
        lax.all_gather(w_uv, "ctx", axis=1, tiled=True),
    )
    nope_dim = up_key.shape[1]
    rope_dim = k_rope.shape[1]
    softmax_scale = (nope_dim + rope_dim) ** (-0.5)
    q_parts = q_nope.reshape(tok_count, head_count, nope_dim)
    q_lat = jnp.einsum("thn,hnl->thl", q_parts, up_key, preferred_element_type=jnp.float32).astype(
        jnp.bfloat16
    )
    q_rot = rotate(q_rope.reshape(tok_count, head_count, rope_dim), positions[:, None]).astype(
        jnp.bfloat16
    )
    k_rot = rotate(k_rope, positions).astype(jnp.bfloat16)
    key_rows = jnp.concatenate([c_kv, k_rot], axis=1)
    queries = jnp.concatenate([q_lat, q_rot], axis=2).reshape(
        tok_count * head_count, latent + rope_dim
    )
    query_pos = jnp.repeat(positions, head_count)
    row_total = tok_count * head_count
    key_part = lax.all_gather(key_rows, "ctx", axis=0, tiled=True)
    key_pos = lax.all_gather(positions, "ctx", axis=0, tiled=True)
    run_max = jnp.full((row_total,), -1e30, jnp.float32)
    scores = (
        jnp.einsum("rk,sk->rs", queries, key_part, preferred_element_type=jnp.float32)
        * softmax_scale
    )
    visible = key_pos[None, :] <= query_pos[:, None]
    new_max = jnp.maximum(run_max, jnp.max(jnp.where(visible, scores, -1e30), axis=1))
    weights = jnp.where(visible, jnp.exp(scores - new_max[:, None]), 0.0)
    new_sum = jnp.sum(weights, axis=1)
    added = jnp.dot(
        weights.astype(jnp.bfloat16), key_part[:, :latent], preferred_element_type=jnp.float32
    )
    o_lat = (added / new_sum[:, None]).astype(jnp.bfloat16).reshape(tok_count, head_count, latent)
    head_out = jnp.einsum("thl,hlv->thv", o_lat, up_value, preferred_element_type=jnp.float32)
    rows_out = head_out.astype(jnp.bfloat16).reshape(tok_count, -1)
    partial_value = jnp.dot(
        lax.all_gather(rows_out, "ctx", axis=0, tiled=True),
        w_out,
        preferred_element_type=jnp.float32,
    )
    summed = lax.psum_scatter(
        partial_value.astype(jnp.bfloat16), "tp", scatter_dimension=0, tiled=True
    )
    return summed


CHUNK_HEADS = 2
RELEASE = -1
EARLY = 1
BEHIND = 1


def on_device(sizes, *args):
    q_nope, q_rope, c_kv, k_rope, positions, w_uk, w_uv, w_out = args
    n, groups, tps = sizes["ctx"], sizes["groups"], sizes["tp"]
    heads = w_uk.shape[0]
    chunks = heads // CHUNK_HEADS
    ends = 3 * chunks // 16
    mids = chunks // 2 - ends
    sz = dict(n=n, g=groups, t=tps, hc=CHUNK_HEADS, ends=ends, mids=mids, tok=q_nope.shape[0],
              release=RELEASE, early=EARLY, behind=BEHIND,
              nope=w_uk.shape[1] * n, rope=k_rope.shape[1], lat=c_kv.shape[1],
              vdim=w_uv.shape[2], tile=w_out.shape[1] // 2)
    seq = n * sz["tok"]
    cols = w_out.shape[1]
    fits = (
        n == 4
        and tps == 4
        and heads % (2 * CHUNK_HEADS) == 0
        and CHUNK_HEADS % groups == 0
        and groups == 2
        and mids >= ends > EARLY
        and mids >= n + 1
        and sz["nope"] == sz["vdim"]
        and seq <= 512
        and seq % (tps * 16) == 0
        and sz["tok"] % (tps * 16) == 0
        and sz["rope"] == 64
        and sz["nope"] % 128 == 0
        and sz["vdim"] % 128 == 0
        and sz["lat"] % 128 == 0
        and cols % 256 == 0
        and w_out.size * 2 + seq * cols * 8 <= 32 * 2**20
    )
    if fits:
        return fast(sz, *args)
    return general(*args)


def solution(mesh):
    in_specs = (
        P(("groups", "ctx"), "tp"),
        P(("groups", "ctx"), "tp"),
        P(("groups", "ctx"), None),
        P(("groups", "ctx"), None),
        P(("groups", "ctx")),
        P("tp", "ctx", None),
        P("tp", "ctx", None),
        P("tp", "ctx"),
    )
    out_specs = P(("groups", "tp"), "ctx")
    return jax.shard_map(
        functools.partial(on_device, dict(mesh.shape)),
        mesh=mesh, in_specs=in_specs, out_specs=out_specs, check_vma=False,
    )
```

```python
import functools
import math

import jax
import jax.numpy as jnp
from jax import lax
from jax.experimental import pallas as pl
from jax.experimental.pallas import tpu as pltpu
from jax.sharding import PartitionSpec as P

F32 = jnp.float32
BF16 = jnp.bfloat16
MESH = pl.DeviceIdType.MESH


def rotate(values, position):
    half_dim = values.shape[-1] // 2
    freqs = 10000.0 ** (-jnp.arange(half_dim, dtype=jnp.float32) / half_dim)
    angles = position.astype(jnp.float32)[..., None] * freqs
    cosine = jnp.cos(angles)
    sine = jnp.sin(angles)
    first_half = values[..., :half_dim].astype(jnp.float32)
    second_half = values[..., half_dim:].astype(jnp.float32)
    return jnp.concatenate(
        [first_half * cosine - second_half * sine, second_half * cosine + first_half * sine],
        axis=-1,
    )


def mega(sz, qn_in, qr_in, kv_in, kr_in, pos_in, wuk_in, wuv_in, wout_in, out_ref,
         qn, qr, kv, kr, pos, wuk, wuv, wout, krot, table, limit, ho, acc, part, got,
         s_w, s_q, s_k, r_w, r_q, r_k, r_p, s_y, r_y, s_t, r_t, s_ag, r_ag, s_rs, r_rs, hop, loc_out):
    n, groups, tps, ends, mids = sz["n"], sz["g"], sz["t"], sz["ends"], sz["mids"]
    tok, hc, nope, rope, lat, vdim = (sz[k] for k in ("tok", "hc", "nope", "rope", "lat", "vdim"))
    scale = (nope + rope) ** (-0.5)
    hg = hc // groups
    c = lax.axis_index("ctx")
    g = lax.axis_index("groups")
    t = lax.axis_index("tp")
    nsl = nope // n
    lsl = lat // n
    share = tok // tps
    seq = n * tok

    def outer(j):
        return jnp.logical_or(j == 0, j == n - 1)

    def count(j):
        return jnp.where(outer(j), ends, mids)

    def begin(j):
        return jnp.where(j == 0, 0, ends + (j - 1) * mids)

    mine = count(c)
    first_mine = begin(c)
    at_end = outer(c)

    def al(x, m):
        return pl.multiple_of(x, m)

    def guard(i, j, body):
        if i < ends:
            body()
        else:
            pl.when(jnp.logical_not(outer(j)))(body)

    def rows_of(s):
        return pl.ds(al(s * tok, tok), tok)

    def piece(kind, i, j, s, part_of):
        if kind in (0, 5):
            src, dst = (kv_in, kv) if kind == 0 else (kr_in, kr)
            if part_of is None:
                return src, dst.at[rows_of(s), :]
            return (src.at[pl.ds(al(part_of * share, share), share), :],
                    dst.at[pl.ds(al(s * tok + part_of * share, share), share), :])
        if kind == 6:
            return pos_in, pos.at[s]
        if kind == 1:
            w = hc * nope
            return (qn_in.at[:, pl.ds(al((begin(j) + i) * w, w), w)],
                    qn.at[rows_of(s), pl.ds(i * w, w)])
        if kind == 2:
            w = hc * rope
            return (qr_in.at[:, pl.ds(al((begin(j) + i) * w, w), w)],
                    qr.at[rows_of(s), pl.ds(i * w, w)])
        if part_of is None:
            src_h, dst_h = pl.ds((begin(j) + i) * hc, hc), pl.ds(i * hc, hc)
        else:
            src_h = pl.ds((begin(j) + i) * hc + part_of * hg, hg)
            dst_h = pl.ds(i * hc + part_of * hg, hg)
        if kind == 3:
            return wuk_in.at[src_h], wuk.at[dst_h, pl.ds(al(s * nsl, nsl), nsl), :]
        return wuv_in.at[src_h], wuv.at[dst_h, pl.ds(al(s * lsl, lsl), lsl), :]

    def copy1(kind, i, d, to=None):
        owner = t if kind in (0, 5) else g
        if to is not None:
            j = to
            src, dst = piece(kind, i, j, c, owner)
        else:
            j = lax.rem(c + n - d, n)
            src, dst = piece(kind, i, c, j, owner)
        if kind in (3, 4):
            send, recv = s_w.at[i], r_w.at[i, d - 1]
        elif kind in (1, 2):
            send, recv = s_q.at[i], r_q.at[i]
        elif kind == 6:
            send, recv = s_k.at[2], r_p
        else:
            send, recv = s_k.at[kind // 5], r_k.at[kind // 5, d - 1]
        return pltpu.make_async_remote_copy(
            src_ref=src, dst_ref=dst, send_sem=send, recv_sem=recv,
            device_id={"ctx": j}, device_id_type=MESH)

    def local(kind, i):
        src, dst = piece(kind, i, c, c, None)
        if kind in (3, 4):
            sem = r_y.at[i]
        elif kind in (1, 2):
            sem = r_q.at[i]
        else:
            sem = r_p if kind == 6 else r_t.at[kind // 5]
        return pltpu.make_async_copy(src, dst, sem)

    def take(ref, sem):
        pltpu.make_async_copy(ref, ref, sem).wait()

    def weight_bytes(blocks):
        return wuk.at[pl.ds(0, blocks), pl.ds(0, nsl), :]

    def query_bytes(blocks):
        return qn.at[pl.ds(0, blocks * tok), pl.ds(0, hc * (nope + rope))]

    def key_bytes(kind, rows):
        return (kr if kind else kv).at[pl.ds(0, rows), :]

    def kinds(i):
        return (0, 1, 2, 3, 4, 5, 6) if i == 0 else (1, 2, 3, 4)

    def turn_of(i, total):
        groups_of = [((3, 4), 0)] if i == 0 else []
        if i + 1 < total:
            groups_of.append(((3, 4), i + 1))
        return groups_of + [((1, 2), i)]

    def send_chunk(b, i, total, targets):
        for group, k in turn_of(i, total):
            for j in targets:
                for kind in group:
                    copy1(kind, k, (j - b) % n, j).start()

    sides = (0, n - 1)

    def far_ends(b):
        if b in sides:
            return [n - 1 - b]
        return [0 if b >= n // 2 else n - 1]

    for i in range(mids):
        def go():
            for kind in kinds(i):
                local(kind, i).start()
        guard(i, c, go)
    wout_copy = pltpu.make_async_copy(wout_in, wout, loc_out)
    wout_copy.start()

    barrier = pltpu.get_barrier_semaphore()

    def tell(sem, axis, to):
        pl.semaphore_signal(sem, inc=1, device_id={axis: to}, device_id_type=MESH)

    pl.when(c > 0)(lambda: tell(barrier, "ctx", c - 1))
    pl.when(c + 1 < n)(lambda: tell(barrier, "ctx", c + 1))
    for axis, me, size in (("groups", g, groups), ("tp", t, tps)):
        for d in range(1, size):
            tell(barrier, axis, lax.rem(me + d, size))
    pl.semaphore_wait(barrier, jnp.where(at_end, 1, 2) + (groups - 1) + (tps - 1))

    def send_keys(b, j):
        for kind in (6, 0, 5):
            copy1(kind, 0, (j - b) % n, j).start()

    for b in range(n):
        @pl.when(c == b)
        def _():
            step = 1 if b < n // 2 else -1
            if b in sides:
                near, next_on, far = (b + k * step for k in range(1, n))
                middle = [next_on, near]
                send_keys(b, near)
                pl.semaphore_wait(hop.at[0], 1)
                send_keys(b, next_on)
                send_chunk(b, 0, mids, middle)
                pl.semaphore_wait(hop.at[1], 1)
                send_keys(b, far)
            else:
                outside, middle, far = b - step, [b + step], b + 2 * step
                for j in (outside, *middle):
                    tell(hop.at[0], "ctx", j)
                send_keys(b, *middle)
                send_chunk(b, 0, mids, middle)
                send_keys(b, outside)
                for i in range(ends):
                    send_chunk(b, i, ends, [outside])
                pl.semaphore_wait(hop.at[0], 1)
                tell(hop.at[1], "ctx", outside)
                send_keys(b, far)
            for i in range(1, mids):
                send_chunk(b, i, mids, middle)
            if b not in sides:
                for i in range(ends):
                    send_chunk(b, i, ends, [far])

    def send_far():
        for b in sides:
            @pl.when(c == b)
            def _():
                for i in range(ends):
                    send_chunk(b, i, ends, far_ends(b))

    def copy_y(kind, i, e, d, sending):
        s = lax.rem(c + n - d, n)
        owner = g if sending else lax.rem(g + groups - e, groups)
        _, dst = piece(kind, i, c, s, owner)
        to = lax.rem(g + e, groups) if sending else owner
        return pltpu.make_async_remote_copy(
            src_ref=dst, dst_ref=dst, send_sem=s_y.at[i], recv_sem=r_y.at[i],
            device_id={"groups": to}, device_id_type=MESH)

    def copy_t(kind, e, d, sending):
        s = lax.rem(c + n - d, n)
        owner = t if sending else lax.rem(t + tps - e, tps)
        _, dst = piece(kind, 0, c, s, owner)
        to = lax.rem(t + e, tps) if sending else owner
        return pltpu.make_async_remote_copy(
            src_ref=dst, dst_ref=dst, send_sem=s_t.at[kind // 5], recv_sem=r_t.at[kind // 5],
            device_id={"tp": to}, device_id_type=MESH)

    def forward_from(i, d):
        take(weight_bytes(2 * hg), r_w.at[i, d - 1])
        for kind in (3, 4):
            for e in range(1, groups):
                copy_y(kind, i, e, d, True).start()

    def forward_weights(i):
        @pl.when(jnp.logical_not(at_end))
        def _():
            forward_from(i, 3)
            forward_from(i, 1)

        forward_from(i, 2)

    def forward_others(near, far):
        for d in (near, far):
            for i in range(ends):
                forward_from(i, d)

    def forward_keys():
        for d in range(1, n):
            for kind in (0, 5):
                copy1(kind, 0, d).wait_recv()
                for e in range(1, tps):
                    copy_t(kind, e, d, True).start()

    wide = 2 * rope

    def turn(x):
        lane = lax.broadcasted_iota(jnp.int32, x.shape, 1)
        low = lax.rem(lane, rope) < rope // 2
        other = jnp.where(low, -pltpu.roll(x, wide - rope // 2, 1), pltpu.roll(x, rope // 2, 1))
        return x * table[0] + other * table[1]

    def tables():
        take(pos, r_p)
        row = jnp.concatenate([pos[s] for s in range(n)], axis=1).astype(F32)
        col = jnp.broadcast_to(row, (wide, seq)).T
        lane = lax.broadcasted_iota(jnp.int32, (1, wide), 1)
        index = lax.rem(lane, rope // 2).astype(F32)
        freqs = jnp.exp(index * (-math.log(10000.0) / (rope // 2)))
        angles = col * freqs
        table[0] = jnp.cos(angles)
        table[1] = jnp.sin(angles)
        limit[...] = jnp.where(row > col[:, :1], -1e30, 3e38)

    def keys():
        for kind in (0, 5):
            take(key_bytes(kind, tok + (n - 1) * (tps - 1) * share), r_t.at[kind // 5])
        raw = kr[...].astype(F32)
        turned = turn(jnp.concatenate([raw, raw], axis=1))
        lane = lax.broadcasted_iota(jnp.int32, turned.shape, 1)
        krot[0] = jnp.where(lane < rope, turned, 0.0).astype(BF16)
        krot[1] = jnp.where(lane < rope, 0.0, turned).astype(BF16)

    def attend(i):
        nt = (((1,), (1,)), ((), ()))

        def pair(p, carry):
            raw = qr[:, pl.ds(al((i * (hc // 2) + p) * wide, wide), wide)]
            qrp = turn(raw.astype(F32)).astype(BF16)
            for k in range(2):
                hl = 2 * p + k
                h = i * hc + hl
                q = qn[:, pl.ds(al(h * nope, nope), nope)]
                ql = jnp.dot(q, wuk[h], preferred_element_type=F32).astype(BF16)
                sc = lax.dot_general(ql, kv[...], nt, preferred_element_type=F32)
                sc = (sc + lax.dot_general(qrp, krot[k], nt, preferred_element_type=F32)) * scale
                sc = jnp.minimum(sc, limit[...])
                w = jnp.exp(sc - jnp.max(sc, axis=1, keepdims=True))
                total = jnp.sum(w, axis=1, keepdims=True)
                o = jnp.dot(w.astype(BF16), kv[...], preferred_element_type=F32)
                o = (o / total).astype(BF16)
                ho[first_mine + i, :, pl.ds(al(hl * vdim, vdim), vdim)] = jnp.dot(
                    o, wuv[h], preferred_element_type=F32).astype(BF16)
            return carry

        lax.fori_loop(0, hc // 2, pair, 0)

    away, stay = 0, 1
    half_rows = seq // 2
    side = t // 2

    def rows_half(h):
        return pl.ds(al((1 - side if h == away else side) * half_rows, half_rows), half_rows)

    def ag_copy(q, h, right):
        ref = ho.at[q, rows_half(h), :]
        return pltpu.make_async_remote_copy(
            src_ref=ref, dst_ref=ref, send_sem=s_ag.at[1 if right else 0],
            recv_sem=r_ag.at[q, h],
            device_id={"ctx": c + 1 if right else c - 1}, device_id_type=MESH)

    inner_right = c < n // 2

    def send_inward(i, h):
        pl.when(inner_right)(lambda: ag_copy(first_mine + i, h, True).start())
        pl.when(jnp.logical_not(inner_right))(lambda: ag_copy(first_mine + i, h, False).start())

    def send_outward(i, h):
        pl.when(jnp.logical_and(inner_right, c > 0))(
            lambda: ag_copy(first_mine + i, h, False).start())
        pl.when(jnp.logical_and(jnp.logical_not(inner_right), c + 1 < n))(
            lambda: ag_copy(first_mine + i, h, True).start())

    cols = acc.shape[1]
    tile = sz["tile"]
    kdim = hc * vdim

    def project(q, rows):
        depth = pl.ds(al(q * kdim, kdim), kdim)

        def step(j, carry):
            at = pl.ds(al(j * tile, tile), tile)
            value = jnp.dot(ho[q, rows, :], wout[depth, at], preferred_element_type=F32)
            acc[rows, at] = acc[rows, at] + value
            return carry

        lax.fori_loop(0, cols // tile, step, 0)

    def arrive(b, i, h, right):
        @pl.when(jnp.logical_and(jnp.logical_and(b >= 0, b < n), jnp.logical_and(i >= 0, i < count(b))))
        def _():
            q = begin(b) + i
            with jax.named_scope("take"):
                ag_copy(q, h, right).wait_recv()
            more = c + 1 < n if right else c > 0
            pl.when(more)(lambda: ag_copy(q, h, right).start())
            project(q, rows_half(h))

    def arrive_all(d, low, high, h):
        def body(i, carry):
            arrive(c + d, i, h, False)
            arrive(c - d, i, h, True)
            return carry

        lax.fori_loop(low, high, body, 0)

    def arrive_inward(i, h):
        pl.when(inner_right)(lambda: arrive(c + 1, i, h, False))
        pl.when(jnp.logical_not(inner_right))(lambda: arrive(c - 1, i, h, True))

    def arrive_outward(i, h):
        pl.when(inner_right)(lambda: arrive(c - 1, i, h, True))
        pl.when(jnp.logical_not(inner_right))(lambda: arrive(c + 1, i, h, False))

    early = sz["early"]

    def chunk(i):
        take(query_bytes(n), r_q.at[i])
        take(weight_bytes((n - 1) * (groups - 1) * 2 * hg + 2 * hc), r_y.at[i])
        attend(i)
        send_outward(i, away)
        send_inward(i, away)
        send_outward(i, stay)
        if i < early:
            pl.when(jnp.logical_not(at_end))(functools.partial(send_inward, i, stay))
        project(first_mine + i, slice(None))

    forward_keys()
    def between():
        tables()
        keys()
        acc[...] = jnp.zeros_like(acc)
        wout_copy.wait()

    @pl.when(jnp.logical_not(at_end))
    def _():
        forward_weights(0)
        between()

    @pl.when(at_end)
    def _():
        between()
        for i in range(sz["release"]):
            arrive_inward(i, away)
            arrive_inward(i, stay)
        send_far()
        pl.when(c == 0)(functools.partial(forward_others, 3, 1))
        pl.when(c == n - 1)(functools.partial(forward_others, 1, 3))
        forward_weights(0)

    for i in range(mids):
        if i + 1 < mids:
            guard(i + 1, c, functools.partial(forward_weights, i + 1))
        guard(i, c, functools.partial(chunk, i))

    def send_late(low, high):
        for i in range(low, high):
            send_inward(i, stay)

    pl.when(at_end)(functools.partial(send_late, 0, ends))
    @pl.when(jnp.logical_not(at_end))
    def _():
        for i in range(early):
            arrive_inward(i, away)
            arrive_inward(i, stay)

    seen = jnp.where(at_end, sz["release"], early)

    def first_away(i, carry):
        arrive_inward(i + seen, away)
        arrive_outward(i - sz["behind"], away)
        return carry

    lax.fori_loop(0, mids + sz["behind"], first_away, 0)
    pl.when(jnp.logical_not(at_end))(functools.partial(send_late, early, mids))

    rows_out = out_ref.shape[0]
    half = cols // 2
    core = lax.rem(t, 2)
    mate = t + 1 - 2 * core
    across = lax.rem(t + 2, tps)
    mate_across = lax.rem(mate + 2, tps)

    def block(r, at):
        return acc[pl.ds(al(r * rows_out, rows_out), rows_out), at]

    def rs_copy(stage, k):
        at = pl.ds(k * half, half)
        slot = (1, 2, 0)[stage]
        return pltpu.make_async_remote_copy(
            src_ref=part.at[slot, :, at], dst_ref=got.at[slot, :, at],
            send_sem=s_rs, recv_sem=r_rs.at[stage, k],
            device_id={"tp": across if stage == 1 else mate}, device_id_type=MESH)

    spans = [slice(k * half, (k + 1) * half) for k in range(2)]

    arrive_all(2, 0, mids, away)
    for i in range(mids):
        guard(i, c, lambda: take(weight_bytes((n - 1) * (groups - 1) * 2 * hg), s_y.at[i]))
    arrive_all(3, 0, ends, away)
    for k, at in enumerate(spans):
        part[1, :, at] = block(mate_across, at).astype(BF16)
        rs_copy(0, k).start()
    arrive_inward(seen, stay)
    arrive_outward(0, stay)
    for k, at in enumerate(spans):
        rs_copy(0, k).wait_recv()
        part[2, :, at] = (block(across, at) + got[1, :, at].astype(F32)).astype(BF16)
        rs_copy(1, k).start()

    def first_stay(i, carry):
        arrive_inward(i + seen, stay)
        arrive_outward(i, stay)
        return carry

    lax.fori_loop(1, mids, first_stay, 0)
    def sent(i, peers):
        take(weight_bytes(peers * 2 * hg), s_w.at[i])
        take(query_bytes(peers), s_q.at[i])

    for i in range(mids):
        if i < ends:
            sent(i, n - 1)
        else:
            pl.when(at_end)(functools.partial(sent, i, n - 2))
            pl.when(jnp.logical_not(at_end))(functools.partial(sent, i, n - 3))
    for kind in (0, 5):
        take(key_bytes(kind, (n - 1) * share), s_k.at[kind // 5])
        take(key_bytes(kind, (n - 1) * (tps - 1) * share), s_t.at[kind // 5])
    take(pos.at[pl.ds(0, n - 1)], s_k.at[2])
    arrive_all(2, 0, mids, stay)

    def drain():
        for b in range(n):
            low = 0 if b == 0 else ends + (b - 1) * mids
            high = low + (ends if b in (0, n - 1) else mids)

            @pl.when(c == b)
            def _():
                if b + 1 < n:
                    take(ho.at[pl.ds(0, high)], s_ag.at[1])
                if b > 0:
                    take(ho.at[pl.ds(low, ho.shape[0] - low)], s_ag.at[0])

    arrive_all(3, 0, ends, stay)
    for k, at in enumerate(spans):
        part[0, :, at] = block(mate, at).astype(BF16)
        rs_copy(2, k).start()
    for k, at in enumerate(spans):
        rs_copy(1, k).wait_recv()
        own = block(t, at) + got[2, :, at].astype(F32)
        rs_copy(2, k).wait_recv()
        out_ref[:, at] = (own + got[0, :, at].astype(F32)).astype(BF16)
    take(part, s_rs)
    drain()


def fast(sz, q_nope, q_rope, c_kv, k_rope, positions, w_uk, w_uv, w_out):
    n, groups, tps, ends, mids = sz["n"], sz["g"], sz["t"], sz["ends"], sz["mids"]
    tok, hc, nope, rope, lat, vdim = (sz[k] for k in ("tok", "hc", "nope", "rope", "lat", "vdim"))
    heads = w_uk.shape[0]
    chunks = heads // hc
    hpc = mids * hc
    seq = n * tok
    cols = w_out.shape[1]
    hbm = pl.BlockSpec(memory_space=pltpu.HBM)
    dma = pltpu.SemaphoreType.DMA
    return pl.pallas_call(
        functools.partial(mega, sz),
        out_shape=pltpu.VMEM((seq // tps, cols), BF16),
        in_specs=[hbm] * 8,
        out_specs=pl.BlockSpec(memory_space=pltpu.VMEM),
        scratch_shapes=[
            pltpu.VMEM((seq, hpc * nope), BF16),
            pltpu.VMEM((seq, hpc * rope), BF16),
            pltpu.VMEM((seq, lat), BF16),
            pltpu.VMEM((seq, rope), BF16),
            pltpu.VMEM((n, 1, tok), jnp.int32),
            pltpu.VMEM((hpc, nope, lat), BF16),
            pltpu.VMEM((hpc, lat, vdim), BF16),
            pltpu.VMEM(w_out.shape, BF16),
            pltpu.VMEM((2, seq, 2 * rope), BF16),
            pltpu.VMEM((2, seq, 2 * rope), F32),
            pltpu.VMEM((seq, seq), F32),
            pltpu.VMEM((chunks, seq, hc * vdim), BF16),
            pltpu.VMEM((seq, cols), F32),
            pltpu.VMEM((tps - 1, seq // tps, cols), BF16),
            pltpu.VMEM((tps - 1, seq // tps, cols), BF16),
            dma((mids,)),
            dma((mids,)),
            dma((3,)),
            dma((mids, n - 1)),
            dma((mids,)),
            dma((2, n - 1)),
            dma,
            dma((mids,)),
            dma((mids,)),
            dma((2,)),
            dma((2,)),
            dma((2,)),
            dma((chunks, 2)),
            dma,
            dma((3, 2)),
            pltpu.SemaphoreType.REGULAR((2,)),
            dma,
        ],
        compiler_params=pltpu.CompilerParams(collective_id=0, has_side_effects=True,
                                             vmem_limit_bytes=60 * 1024 * 1024),
    )(q_nope, q_rope, c_kv, k_rope, positions.reshape(1, tok), w_uk, w_uv, w_out)


def general(q_nope, q_rope, c_kv, k_rope, positions, w_uk, w_uv, w_out):
    tok_count = q_nope.shape[0]
    head_count = w_uk.shape[0]
    latent = c_kv.shape[1]
    up_key, up_value = (
        lax.all_gather(w_uk, "ctx", axis=1, tiled=True),
        lax.all_gather(w_uv, "ctx", axis=1, tiled=True),
    )
    nope_dim = up_key.shape[1]
    rope_dim = k_rope.shape[1]
    softmax_scale = (nope_dim + rope_dim) ** (-0.5)
    q_parts = q_nope.reshape(tok_count, head_count, nope_dim)
    q_lat = jnp.einsum("thn,hnl->thl", q_parts, up_key, preferred_element_type=jnp.float32).astype(
        jnp.bfloat16
    )
    q_rot = rotate(q_rope.reshape(tok_count, head_count, rope_dim), positions[:, None]).astype(
        jnp.bfloat16
    )
    k_rot = rotate(k_rope, positions).astype(jnp.bfloat16)
    key_rows = jnp.concatenate([c_kv, k_rot], axis=1)
    queries = jnp.concatenate([q_lat, q_rot], axis=2).reshape(
        tok_count * head_count, latent + rope_dim
    )
    query_pos = jnp.repeat(positions, head_count)
    row_total = tok_count * head_count
    key_part = lax.all_gather(key_rows, "ctx", axis=0, tiled=True)
    key_pos = lax.all_gather(positions, "ctx", axis=0, tiled=True)
    run_max = jnp.full((row_total,), -1e30, jnp.float32)
    scores = (
        jnp.einsum("rk,sk->rs", queries, key_part, preferred_element_type=jnp.float32)
        * softmax_scale
    )
    visible = key_pos[None, :] <= query_pos[:, None]
    new_max = jnp.maximum(run_max, jnp.max(jnp.where(visible, scores, -1e30), axis=1))
    weights = jnp.where(visible, jnp.exp(scores - new_max[:, None]), 0.0)
    new_sum = jnp.sum(weights, axis=1)
    added = jnp.dot(
        weights.astype(jnp.bfloat16), key_part[:, :latent], preferred_element_type=jnp.float32
    )
    o_lat = (added / new_sum[:, None]).astype(jnp.bfloat16).reshape(tok_count, head_count, latent)
    head_out = jnp.einsum("thl,hlv->thv", o_lat, up_value, preferred_element_type=jnp.float32)
    rows_out = head_out.astype(jnp.bfloat16).reshape(tok_count, -1)
    partial_value = jnp.dot(
        lax.all_gather(rows_out, "ctx", axis=0, tiled=True),
        w_out,
        preferred_element_type=jnp.float32,
    )
    summed = lax.psum_scatter(
        partial_value.astype(jnp.bfloat16), "tp", scatter_dimension=0, tiled=True
    )
    return summed


CHUNK_HEADS = 2
END_CHUNKS = 2
RELEASE = 3
EARLY = 1
BEHIND = 1


def on_device(sizes, *args):
    q_nope, q_rope, c_kv, k_rope, positions, w_uk, w_uv, w_out = args
    n, groups, tps = sizes["ctx"], sizes["groups"], sizes["tp"]
    heads = w_uk.shape[0]
    chunks = heads // CHUNK_HEADS
    ends = END_CHUNKS * chunks // 16
    mids = chunks // 2 - ends
    sz = dict(n=n, g=groups, t=tps, hc=CHUNK_HEADS, ends=ends, mids=mids, tok=q_nope.shape[0],
              release=RELEASE, early=EARLY, behind=BEHIND,
              nope=w_uk.shape[1] * n, rope=k_rope.shape[1], lat=c_kv.shape[1],
              vdim=w_uv.shape[2], tile=w_out.shape[1] // 2)
    seq = n * sz["tok"]
    cols = w_out.shape[1]
    fits = (
        n == 4
        and tps == 4
        and heads % (2 * CHUNK_HEADS) == 0
        and CHUNK_HEADS % groups == 0
        and groups == 2
        and mids >= ends > EARLY
        and mids > RELEASE
        and mids >= n + 1
        and sz["nope"] == sz["vdim"]
        and seq <= 512
        and seq % (tps * 16) == 0
        and sz["tok"] % (tps * 16) == 0
        and sz["rope"] == 64
        and sz["nope"] % 128 == 0
        and sz["vdim"] % 128 == 0
        and sz["lat"] % 128 == 0
        and cols % 256 == 0
        and w_out.size * 2 + seq * cols * 8 <= 32 * 2**20
    )
    if fits:
        return fast(sz, *args)
    return general(*args)


def solution(mesh):
    in_specs = (
        P(("groups", "ctx"), "tp"),
        P(("groups", "ctx"), "tp"),
        P(("groups", "ctx"), None),
        P(("groups", "ctx"), None),
        P(("groups", "ctx")),
        P("tp", "ctx", None),
        P("tp", "ctx", None),
        P("tp", "ctx"),
    )
    out_specs = P(("groups", "tp"), "ctx")
    return jax.shard_map(
        functools.partial(on_device, dict(mesh.shape)),
        mesh=mesh, in_specs=in_specs, out_specs=out_specs, check_vma=False,
    )
```

```python
import functools
import math

import jax
import jax.numpy as jnp
from jax import lax
from jax.experimental import pallas as pl
from jax.experimental.pallas import tpu as pltpu
from jax.sharding import PartitionSpec as P

F32 = jnp.float32
BF16 = jnp.bfloat16
MESH = pl.DeviceIdType.MESH


def rotate(values, position):
    half_dim = values.shape[-1] // 2
    freqs = 10000.0 ** (-jnp.arange(half_dim, dtype=jnp.float32) / half_dim)
    angles = position.astype(jnp.float32)[..., None] * freqs
    cosine = jnp.cos(angles)
    sine = jnp.sin(angles)
    first_half = values[..., :half_dim].astype(jnp.float32)
    second_half = values[..., half_dim:].astype(jnp.float32)
    return jnp.concatenate(
        [first_half * cosine - second_half * sine, second_half * cosine + first_half * sine],
        axis=-1,
    )


def mega(sz, qn_in, qr_in, kv_in, kr_in, pos_in, wuk_in, wuv_in, wout_in, out_ref,
         qn, qr, kv, kr, pos, wuk, wuv, wout, krot, table, limit, ho, acc, part, got,
         s_w, s_q, s_k, r_w, r_q, r_k, r_p, s_y, r_y, s_t, r_t, s_ag, r_ag, s_rs, r_rs, hop, loc_out):
    n, groups, tps, ends, mids = sz["n"], sz["g"], sz["t"], sz["ends"], sz["mids"]
    tok, hc, nope, rope, lat, vdim = (sz[k] for k in ("tok", "hc", "nope", "rope", "lat", "vdim"))
    scale = (nope + rope) ** (-0.5)
    hg = hc // groups
    c = lax.axis_index("ctx")
    g = lax.axis_index("groups")
    t = lax.axis_index("tp")
    nsl = nope // n
    lsl = lat // n
    share = tok // tps
    seq = n * tok

    def outer(j):
        return jnp.logical_or(j == 0, j == n - 1)

    def count(j):
        return jnp.where(outer(j), ends, mids)

    def begin(j):
        return jnp.where(j == 0, 0, ends + (j - 1) * mids)

    mine = count(c)
    first_mine = begin(c)
    at_end = outer(c)

    def al(x, m):
        return pl.multiple_of(x, m)

    def guard(i, j, body):
        if i < ends:
            body()
        else:
            pl.when(jnp.logical_not(outer(j)))(body)

    def rows_of(s):
        return pl.ds(al(s * tok, tok), tok)

    def piece(kind, i, j, s, part_of):
        if kind in (0, 5):
            src, dst = (kv_in, kv) if kind == 0 else (kr_in, kr)
            if part_of is None:
                return src, dst.at[rows_of(s), :]
            return (src.at[pl.ds(al(part_of * share, share), share), :],
                    dst.at[pl.ds(al(s * tok + part_of * share, share), share), :])
        if kind == 6:
            return pos_in, pos.at[s]
        if kind == 1:
            w = hc * nope
            return (qn_in.at[:, pl.ds(al((begin(j) + i) * w, w), w)],
                    qn.at[rows_of(s), pl.ds(i * w, w)])
        if kind == 2:
            w = hc * rope
            return (qr_in.at[:, pl.ds(al((begin(j) + i) * w, w), w)],
                    qr.at[rows_of(s), pl.ds(i * w, w)])
        if part_of is None:
            src_h, dst_h = pl.ds((begin(j) + i) * hc, hc), pl.ds(i * hc, hc)
        else:
            src_h = pl.ds((begin(j) + i) * hc + part_of * hg, hg)
            dst_h = pl.ds(i * hc + part_of * hg, hg)
        if kind == 3:
            return wuk_in.at[src_h], wuk.at[dst_h, pl.ds(al(s * nsl, nsl), nsl), :]
        return wuv_in.at[src_h], wuv.at[dst_h, pl.ds(al(s * lsl, lsl), lsl), :]

    def copy1(kind, i, d, to=None):
        owner = t if kind in (0, 5) else g
        if to is not None:
            j = to
            src, dst = piece(kind, i, j, c, owner)
        else:
            j = lax.rem(c + n - d, n)
            src, dst = piece(kind, i, c, j, owner)
        if kind in (3, 4):
            send, recv = s_w.at[i], r_w.at[i, d - 1]
        elif kind in (1, 2):
            send, recv = s_q.at[i], r_q.at[i]
        elif kind == 6:
            send, recv = s_k.at[2], r_p
        else:
            send, recv = s_k.at[kind // 5], r_k.at[kind // 5, d - 1]
        return pltpu.make_async_remote_copy(
            src_ref=src, dst_ref=dst, send_sem=send, recv_sem=recv,
            device_id={"ctx": j}, device_id_type=MESH)

    def local(kind, i):
        src, dst = piece(kind, i, c, c, None)
        if kind in (3, 4):
            sem = r_y.at[i]
        elif kind in (1, 2):
            sem = r_q.at[i]
        else:
            sem = r_p if kind == 6 else r_t.at[kind // 5]
        return pltpu.make_async_copy(src, dst, sem)

    def take(ref, sem):
        pltpu.make_async_copy(ref, ref, sem).wait()

    def weight_bytes(blocks):
        return wuk.at[pl.ds(0, blocks), pl.ds(0, nsl), :]

    def query_bytes(blocks):
        return qn.at[pl.ds(0, blocks * tok), pl.ds(0, hc * (nope + rope))]

    def key_bytes(kind, rows):
        return (kr if kind else kv).at[pl.ds(0, rows), :]

    def kinds(i):
        return (0, 1, 2, 3, 4, 5, 6) if i == 0 else (1, 2, 3, 4)

    def turn_of(i, total):
        groups_of = [((3, 4), 0)] if i == 0 else []
        if i + 1 < total:
            groups_of.append(((3, 4), i + 1))
        return groups_of + [((1, 2), i)]

    def send_chunk(b, i, total, targets):
        for group, k in turn_of(i, total):
            for j in targets:
                for kind in group:
                    copy1(kind, k, (j - b) % n, j).start()

    sides = (0, n - 1)

    def send_far_chunk(b, k, far):
        for kind in (3, 4, 1, 2):
            copy1(kind, k, (far - b) % n, far).start()

    for i in range(mids):
        def go():
            for kind in kinds(i):
                local(kind, i).start()
        guard(i, c, go)
    wout_copy = pltpu.make_async_copy(wout_in, wout, loc_out)
    wout_copy.start()

    barrier = pltpu.get_barrier_semaphore()

    def tell(sem, axis, to):
        pl.semaphore_signal(sem, inc=1, device_id={axis: to}, device_id_type=MESH)

    pl.when(c > 0)(lambda: tell(barrier, "ctx", c - 1))
    pl.when(c + 1 < n)(lambda: tell(barrier, "ctx", c + 1))
    for axis, me, size in (("groups", g, groups), ("tp", t, tps)):
        for d in range(1, size):
            tell(barrier, axis, lax.rem(me + d, size))
    pl.semaphore_wait(barrier, jnp.where(at_end, 1, 2) + (groups - 1) + (tps - 1))

    def send_keys(b, j, group):
        for kind in group:
            copy1(kind, 0, (j - b) % n, j).start()

    for b in range(n):
        @pl.when(c == b)
        def _():
            step = 1 if b < n // 2 else -1
            if b in sides:
                near, next_on, far = (b + k * step for k in range(1, n))
                middle = [next_on, near]
                send_keys(b, near, (6, 0, 5))
                pl.semaphore_wait(hop.at[0], 1)
                send_keys(b, next_on, (6, 0, 5))
                send_chunk(b, 0, mids, middle)
                pl.semaphore_wait(hop.at[1], 1)
                send_keys(b, far, (6,))
            else:
                outside, middle, far = b - step, [b + step], b + 2 * step
                for j in (outside, *middle):
                    tell(hop.at[0], "ctx", j)
                send_keys(b, middle[0], (6, 0, 5))
                send_chunk(b, 0, mids, middle)
                send_keys(b, outside, (6, 0, 5))
                for i in range(ends):
                    send_chunk(b, i, ends, [outside])
                pl.semaphore_wait(hop.at[0], 1)
                tell(hop.at[1], "ctx", outside)
                send_keys(b, far, (6,))
            for i in range(1, mids):
                send_chunk(b, i, mids, middle)
                if b not in sides:
                    for k in range(ends):
                        if i == mids - 1 - (ends - 1 - k) * sz["spread"]:
                            send_far_chunk(b, k, far)

    def send_far(k):
        for b in sides:
            pl.when(c == b)(functools.partial(send_far_chunk, b, k, n - 1 - b))

    def copy_y(kind, i, e, d, sending):
        s = lax.rem(c + n - d, n)
        owner = g if sending else lax.rem(g + groups - e, groups)
        _, dst = piece(kind, i, c, s, owner)
        to = lax.rem(g + e, groups) if sending else owner
        return pltpu.make_async_remote_copy(
            src_ref=dst, dst_ref=dst, send_sem=s_y.at[i], recv_sem=r_y.at[i],
            device_id={"groups": to}, device_id_type=MESH)

    def copy_t(kind, e, d, sending):
        s = lax.rem(c + n - d, n)
        owner = t if sending else lax.rem(t + tps - e, tps)
        _, dst = piece(kind, 0, c, s, owner)
        to = lax.rem(t + e, tps) if sending else owner
        return pltpu.make_async_remote_copy(
            src_ref=dst, dst_ref=dst, send_sem=s_t.at[kind // 5], recv_sem=r_t.at[kind // 5],
            device_id={"tp": to}, device_id_type=MESH)

    def forward_from(i, d):
        take(weight_bytes(2 * hg), r_w.at[i, d - 1])
        for kind in (3, 4):
            for e in range(1, groups):
                copy_y(kind, i, e, d, True).start()

    def forward_weights(i):
        @pl.when(jnp.logical_not(at_end))
        def _():
            forward_from(i, 3)
            forward_from(i, 1)

        forward_from(i, 2)

    def forward_others(near, far):
        for d in (near, far):
            for i in range(ends):
                forward_from(i, d)

    def pass_key(kind, b, origin, out):
        ref = (kr if kind else kv).at[pl.ds(al(origin * tok + t * share, share), share), :]
        return pltpu.make_async_remote_copy(
            src_ref=ref, dst_ref=ref, send_sem=s_k.at[kind // 5],
            recv_sem=r_k.at[kind // 5, (out - origin) % n - 1],
            device_id={"ctx": out}, device_id_type=MESH)

    def forward_keys():
        for d in range(1, n):
            for kind in (0, 5):
                copy1(kind, 0, d).wait_recv()
                for b in range(1, n - 1):
                    out = 0 if b < n // 2 else n - 1
                    if (b - d) % n != out:
                        pl.when(c == b)(lambda: pass_key(kind, b, (b - d) % n, out).start())
                for e in range(1, tps):
                    copy_t(kind, e, d, True).start()

    wide = 2 * rope

    def turn(x):
        lane = lax.broadcasted_iota(jnp.int32, x.shape, 1)
        low = lax.rem(lane, rope) < rope // 2
        other = jnp.where(low, -pltpu.roll(x, wide - rope // 2, 1), pltpu.roll(x, rope // 2, 1))
        return x * table[0] + other * table[1]

    def tables():
        take(pos, r_p)
        row = jnp.concatenate([pos[s] for s in range(n)], axis=1).astype(F32)
        col = jnp.broadcast_to(row, (wide, seq)).T
        lane = lax.broadcasted_iota(jnp.int32, (1, wide), 1)
        index = lax.rem(lane, rope // 2).astype(F32)
        freqs = jnp.exp(index * (-math.log(10000.0) / (rope // 2)))
        angles = col * freqs
        table[0] = jnp.cos(angles)
        table[1] = jnp.sin(angles)
        limit[...] = jnp.where(row > col[:, :1], -1e30, 3e38)

    def keys():
        for kind in (0, 5):
            take(key_bytes(kind, tok + (n - 1) * (tps - 1) * share), r_t.at[kind // 5])
        raw = kr[...].astype(F32)
        turned = turn(jnp.concatenate([raw, raw], axis=1))
        lane = lax.broadcasted_iota(jnp.int32, turned.shape, 1)
        krot[0] = jnp.where(lane < rope, turned, 0.0).astype(BF16)
        krot[1] = jnp.where(lane < rope, 0.0, turned).astype(BF16)

    def attend(i):
        nt = (((1,), (1,)), ((), ()))

        def pair(p, carry):
            raw = qr[:, pl.ds(al((i * (hc // 2) + p) * wide, wide), wide)]
            qrp = turn(raw.astype(F32)).astype(BF16)
            for k in range(2):
                hl = 2 * p + k
                h = i * hc + hl
                q = qn[:, pl.ds(al(h * nope, nope), nope)]
                ql = jnp.dot(q, wuk[h], preferred_element_type=F32).astype(BF16)
                sc = lax.dot_general(ql, kv[...], nt, preferred_element_type=F32)
                sc = (sc + lax.dot_general(qrp, krot[k], nt, preferred_element_type=F32)) * scale
                sc = jnp.minimum(sc, limit[...])
                w = jnp.exp(sc - jnp.max(sc, axis=1, keepdims=True))
                total = jnp.sum(w, axis=1, keepdims=True)
                o = jnp.dot(w.astype(BF16), kv[...], preferred_element_type=F32)
                o = (o / total).astype(BF16)
                ho[first_mine + i, :, pl.ds(al(hl * vdim, vdim), vdim)] = jnp.dot(
                    o, wuv[h], preferred_element_type=F32).astype(BF16)
            return carry

        lax.fori_loop(0, hc // 2, pair, 0)

    away, stay = 0, 1
    half_rows = seq // 2
    side = t // 2

    def rows_half(h):
        return pl.ds(al((1 - side if h == away else side) * half_rows, half_rows), half_rows)

    quarter = half_rows // 2

    def parts_of(h):
        return (0,) if h == away else (1, 2)

    def ag_copy(q, p, right):
        rows = rows_half(away)
        if p > 0:
            rows = pl.ds(al(side * half_rows + (p - 1) * quarter, quarter), quarter)
        ref = ho.at[q, rows, :]
        return pltpu.make_async_remote_copy(
            src_ref=ref, dst_ref=ref, send_sem=s_ag.at[1 if right else 0],
            recv_sem=r_ag.at[q, p],
            device_id={"ctx": c + 1 if right else c - 1}, device_id_type=MESH)

    inner_right = c < n // 2

    def send_item(i, h, right):
        for p in parts_of(h):
            ag_copy(first_mine + i, p, right).start()

    def send_inward(i, h):
        pl.when(inner_right)(functools.partial(send_item, i, h, True))
        pl.when(jnp.logical_not(inner_right))(functools.partial(send_item, i, h, False))

    def send_outward(i, h):
        pl.when(jnp.logical_and(inner_right, c > 0))(functools.partial(send_item, i, h, False))
        pl.when(jnp.logical_and(jnp.logical_not(inner_right), c + 1 < n))(
            functools.partial(send_item, i, h, True))

    cols = acc.shape[1]
    tile = sz["tile"]
    kdim = hc * vdim

    def project(q, rows):
        depth = pl.ds(al(q * kdim, kdim), kdim)

        def step(j, carry):
            at = pl.ds(al(j * tile, tile), tile)
            value = jnp.dot(ho[q, rows, :], wout[depth, at], preferred_element_type=F32)
            acc[rows, at] = acc[rows, at] + value
            return carry

        lax.fori_loop(0, cols // tile, step, 0)

    def arrive(b, i, h, right):
        @pl.when(jnp.logical_and(jnp.logical_and(b >= 0, b < n), jnp.logical_and(i >= 0, i < count(b))))
        def _():
            q = begin(b) + i
            more = c + 1 < n if right else c > 0
            for p in parts_of(h):
                with jax.named_scope("take"):
                    ag_copy(q, p, right).wait_recv()
                pl.when(more)(lambda: ag_copy(q, p, right).start())
            project(q, rows_half(h))

    def arrive_all(d, low, high, h):
        def body(i, carry):
            arrive(c + d, i, h, False)
            arrive(c - d, i, h, True)
            return carry

        lax.fori_loop(low, high, body, 0)

    def arrive_inward(i, h):
        pl.when(inner_right)(lambda: arrive(c + 1, i, h, False))
        pl.when(jnp.logical_not(inner_right))(lambda: arrive(c - 1, i, h, True))

    def arrive_outward(i, h):
        pl.when(inner_right)(lambda: arrive(c - 1, i, h, True))
        pl.when(jnp.logical_not(inner_right))(lambda: arrive(c + 1, i, h, False))

    early = sz["early"]

    def chunk(i):
        take(query_bytes(n), r_q.at[i])
        take(weight_bytes((n - 1) * (groups - 1) * 2 * hg + 2 * hc), r_y.at[i])
        attend(i)
        send_outward(i, away)
        send_inward(i, away)
        send_outward(i, stay)
        if i < early:
            pl.when(jnp.logical_not(at_end))(functools.partial(send_inward, i, stay))
        project(first_mine + i, slice(None))

    forward_keys()
    def between():
        tables()
        keys()
        acc[...] = jnp.zeros_like(acc)
        wout_copy.wait()

    @pl.when(jnp.logical_not(at_end))
    def _():
        forward_weights(0)
        between()

    @pl.when(at_end)
    def _():
        between()
        for i in range(sz["release"]):
            arrive_inward(i, away)
            arrive_inward(i, stay)
            for k in range(ends):
                if i == sz["release"] - 1 - (ends - 1 - k) * sz["gap"]:
                    send_far(k)
        pl.when(c == 0)(functools.partial(forward_others, 3, 1))
        pl.when(c == n - 1)(functools.partial(forward_others, 1, 3))
        forward_weights(0)

    for i in range(mids):
        if i + 1 < mids:
            guard(i + 1, c, functools.partial(forward_weights, i + 1))
        guard(i, c, functools.partial(chunk, i))

    def send_late(low, high):
        for i in range(low, high):
            send_inward(i, stay)

    pl.when(at_end)(functools.partial(send_late, 0, ends))
    @pl.when(jnp.logical_not(at_end))
    def _():
        for i in range(early):
            arrive_inward(i, away)
            arrive_inward(i, stay)

    seen = jnp.where(at_end, sz["release"], early)

    def first_away(i, carry):
        arrive_inward(i + seen, away)
        arrive_outward(i - sz["behind"], away)
        return carry

    lax.fori_loop(0, mids + sz["behind"], first_away, 0)
    pl.when(jnp.logical_not(at_end))(functools.partial(send_late, early, mids))

    rows_out = out_ref.shape[0]
    half = cols // 2
    core = lax.rem(t, 2)
    mate = t + 1 - 2 * core
    across = lax.rem(t + 2, tps)
    mate_across = lax.rem(mate + 2, tps)

    def block(r, at):
        return acc[pl.ds(al(r * rows_out, rows_out), rows_out), at]

    def rs_copy(stage, k):
        at = pl.ds(k * half, half)
        slot = (1, 2, 0)[stage]
        return pltpu.make_async_remote_copy(
            src_ref=part.at[slot, :, at], dst_ref=got.at[slot, :, at],
            send_sem=s_rs, recv_sem=r_rs.at[stage, k],
            device_id={"tp": across if stage == 1 else mate}, device_id_type=MESH)

    spans = [slice(k * half, (k + 1) * half) for k in range(2)]

    arrive_all(2, 0, mids, away)
    for i in range(mids):
        guard(i, c, lambda: take(weight_bytes((n - 1) * (groups - 1) * 2 * hg), s_y.at[i]))
    arrive_all(3, 0, ends, away)
    for k, at in enumerate(spans):
        part[1, :, at] = block(mate_across, at).astype(BF16)
        rs_copy(0, k).start()
    arrive_inward(seen, stay)
    arrive_outward(0, stay)
    for k, at in enumerate(spans):
        rs_copy(0, k).wait_recv()
        part[2, :, at] = (block(across, at) + got[1, :, at].astype(F32)).astype(BF16)
        rs_copy(1, k).start()

    def first_stay(i, carry):
        arrive_inward(i + seen, stay)
        arrive_outward(i, stay)
        return carry

    lax.fori_loop(1, mids, first_stay, 0)
    def sent(i, peers):
        take(weight_bytes(peers * 2 * hg), s_w.at[i])
        take(query_bytes(peers), s_q.at[i])

    for i in range(mids):
        if i < ends:
            sent(i, n - 1)
        else:
            pl.when(at_end)(functools.partial(sent, i, n - 2))
            pl.when(jnp.logical_not(at_end))(functools.partial(sent, i, n - 3))
    for kind in (0, 5):
        pl.when(at_end)(lambda: take(key_bytes(kind, 2 * share), s_k.at[kind // 5]))
        pl.when(jnp.logical_not(at_end))(lambda: take(key_bytes(kind, 4 * share), s_k.at[kind // 5]))
        take(key_bytes(kind, (n - 1) * (tps - 1) * share), s_t.at[kind // 5])
    take(pos.at[pl.ds(0, n - 1)], s_k.at[2])
    arrive_all(2, 0, mids, stay)

    def drain():
        for b in range(n):
            low = 0 if b == 0 else ends + (b - 1) * mids
            high = low + (ends if b in (0, n - 1) else mids)

            @pl.when(c == b)
            def _():
                if b + 1 < n:
                    take(ho.at[pl.ds(0, high)], s_ag.at[1])
                if b > 0:
                    take(ho.at[pl.ds(low, ho.shape[0] - low)], s_ag.at[0])

    arrive_all(3, 0, ends, stay)
    for k, at in enumerate(spans):
        part[0, :, at] = block(mate, at).astype(BF16)
        rs_copy(2, k).start()
    for k, at in enumerate(spans):
        rs_copy(1, k).wait_recv()
        own = block(t, at) + got[2, :, at].astype(F32)
        rs_copy(2, k).wait_recv()
        out_ref[:, at] = (own + got[0, :, at].astype(F32)).astype(BF16)
    take(part, s_rs)
    drain()


def fast(sz, q_nope, q_rope, c_kv, k_rope, positions, w_uk, w_uv, w_out):
    n, groups, tps, ends, mids = sz["n"], sz["g"], sz["t"], sz["ends"], sz["mids"]
    tok, hc, nope, rope, lat, vdim = (sz[k] for k in ("tok", "hc", "nope", "rope", "lat", "vdim"))
    heads = w_uk.shape[0]
    chunks = heads // hc
    hpc = mids * hc
    seq = n * tok
    cols = w_out.shape[1]
    hbm = pl.BlockSpec(memory_space=pltpu.HBM)
    dma = pltpu.SemaphoreType.DMA
    return pl.pallas_call(
        functools.partial(mega, sz),
        out_shape=pltpu.VMEM((seq // tps, cols), BF16),
        in_specs=[hbm] * 8,
        out_specs=pl.BlockSpec(memory_space=pltpu.VMEM),
        scratch_shapes=[
            pltpu.VMEM((seq, hpc * nope), BF16),
            pltpu.VMEM((seq, hpc * rope), BF16),
            pltpu.VMEM((seq, lat), BF16),
            pltpu.VMEM((seq, rope), BF16),
            pltpu.VMEM((n, 1, tok), jnp.int32),
            pltpu.VMEM((hpc, nope, lat), BF16),
            pltpu.VMEM((hpc, lat, vdim), BF16),
            pltpu.VMEM(w_out.shape, BF16),
            pltpu.VMEM((2, seq, 2 * rope), BF16),
            pltpu.VMEM((2, seq, 2 * rope), F32),
            pltpu.VMEM((seq, seq), F32),
            pltpu.VMEM((chunks, seq, hc * vdim), BF16),
            pltpu.VMEM((seq, cols), F32),
            pltpu.VMEM((tps - 1, seq // tps, cols), BF16),
            pltpu.VMEM((tps - 1, seq // tps, cols), BF16),
            dma((mids,)),
            dma((mids,)),
            dma((3,)),
            dma((mids, n - 1)),
            dma((mids,)),
            dma((2, n - 1)),
            dma,
            dma((mids,)),
            dma((mids,)),
            dma((2,)),
            dma((2,)),
            dma((2,)),
            dma((chunks, 3)),
            dma,
            dma((3, 2)),
            pltpu.SemaphoreType.REGULAR((2,)),
            dma,
        ],
        compiler_params=pltpu.CompilerParams(collective_id=0, has_side_effects=True,
                                             vmem_limit_bytes=60 * 1024 * 1024),
    )(q_nope, q_rope, c_kv, k_rope, positions.reshape(1, tok), w_uk, w_uv, w_out)


def general(q_nope, q_rope, c_kv, k_rope, positions, w_uk, w_uv, w_out):
    tok_count = q_nope.shape[0]
    head_count = w_uk.shape[0]
    latent = c_kv.shape[1]
    up_key, up_value = (
        lax.all_gather(w_uk, "ctx", axis=1, tiled=True),
        lax.all_gather(w_uv, "ctx", axis=1, tiled=True),
    )
    nope_dim = up_key.shape[1]
    rope_dim = k_rope.shape[1]
    softmax_scale = (nope_dim + rope_dim) ** (-0.5)
    q_parts = q_nope.reshape(tok_count, head_count, nope_dim)
    q_lat = jnp.einsum("thn,hnl->thl", q_parts, up_key, preferred_element_type=jnp.float32).astype(
        jnp.bfloat16
    )
    q_rot = rotate(q_rope.reshape(tok_count, head_count, rope_dim), positions[:, None]).astype(
        jnp.bfloat16
    )
    k_rot = rotate(k_rope, positions).astype(jnp.bfloat16)
    key_rows = jnp.concatenate([c_kv, k_rot], axis=1)
    queries = jnp.concatenate([q_lat, q_rot], axis=2).reshape(
        tok_count * head_count, latent + rope_dim
    )
    query_pos = jnp.repeat(positions, head_count)
    row_total = tok_count * head_count
    key_part = lax.all_gather(key_rows, "ctx", axis=0, tiled=True)
    key_pos = lax.all_gather(positions, "ctx", axis=0, tiled=True)
    run_max = jnp.full((row_total,), -1e30, jnp.float32)
    scores = (
        jnp.einsum("rk,sk->rs", queries, key_part, preferred_element_type=jnp.float32)
        * softmax_scale
    )
    visible = key_pos[None, :] <= query_pos[:, None]
    new_max = jnp.maximum(run_max, jnp.max(jnp.where(visible, scores, -1e30), axis=1))
    weights = jnp.where(visible, jnp.exp(scores - new_max[:, None]), 0.0)
    new_sum = jnp.sum(weights, axis=1)
    added = jnp.dot(
        weights.astype(jnp.bfloat16), key_part[:, :latent], preferred_element_type=jnp.float32
    )
    o_lat = (added / new_sum[:, None]).astype(jnp.bfloat16).reshape(tok_count, head_count, latent)
    head_out = jnp.einsum("thl,hlv->thv", o_lat, up_value, preferred_element_type=jnp.float32)
    rows_out = head_out.astype(jnp.bfloat16).reshape(tok_count, -1)
    partial_value = jnp.dot(
        lax.all_gather(rows_out, "ctx", axis=0, tiled=True),
        w_out,
        preferred_element_type=jnp.float32,
    )
    summed = lax.psum_scatter(
        partial_value.astype(jnp.bfloat16), "tp", scatter_dimension=0, tiled=True
    )
    return summed


CHUNK_HEADS = 2
END_CHUNKS = 2
RELEASE = 4
SPREAD = 2
GAP = 2
EARLY = 1
BEHIND = 1


def on_device(sizes, *args):
    q_nope, q_rope, c_kv, k_rope, positions, w_uk, w_uv, w_out = args
    n, groups, tps = sizes["ctx"], sizes["groups"], sizes["tp"]
    heads = w_uk.shape[0]
    chunks = heads // CHUNK_HEADS
    ends = END_CHUNKS * chunks // 16
    mids = chunks // 2 - ends
    sz = dict(n=n, g=groups, t=tps, hc=CHUNK_HEADS, ends=ends, mids=mids, tok=q_nope.shape[0],
              release=RELEASE, spread=SPREAD, gap=GAP, early=EARLY, behind=BEHIND,
              nope=w_uk.shape[1] * n, rope=k_rope.shape[1], lat=c_kv.shape[1],
              vdim=w_uv.shape[2], tile=w_out.shape[1] // 2)
    seq = n * sz["tok"]
    cols = w_out.shape[1]
    fits = (
        n == 4
        and tps == 4
        and heads % (2 * CHUNK_HEADS) == 0
        and CHUNK_HEADS % groups == 0
        and groups == 2
        and mids >= ends > EARLY
        and mids > RELEASE > (ends - 1) * GAP
        and mids - 1 > (ends - 1) * SPREAD
        and mids >= n + 1
        and sz["nope"] == sz["vdim"]
        and seq <= 512
        and seq % (tps * 16) == 0
        and sz["tok"] % (tps * 16) == 0
        and sz["rope"] == 64
        and sz["nope"] % 128 == 0
        and sz["vdim"] % 128 == 0
        and sz["lat"] % 128 == 0
        and cols % 256 == 0
        and w_out.size * 2 + seq * cols * 8 <= 32 * 2**20
    )
    if fits:
        return fast(sz, *args)
    return general(*args)


def solution(mesh):
    in_specs = (
        P(("groups", "ctx"), "tp"),
        P(("groups", "ctx"), "tp"),
        P(("groups", "ctx"), None),
        P(("groups", "ctx"), None),
        P(("groups", "ctx")),
        P("tp", "ctx", None),
        P("tp", "ctx", None),
        P("tp", "ctx"),
    )
    out_specs = P(("groups", "tp"), "ctx")
    return jax.shard_map(
        functools.partial(on_device, dict(mesh.shape)),
        mesh=mesh, in_specs=in_specs, out_specs=out_specs, check_vma=False,
    )
```

```python
import functools
import math

import jax
import jax.numpy as jnp
from jax import lax
from jax.experimental import pallas as pl
from jax.experimental.pallas import tpu as pltpu
from jax.sharding import PartitionSpec as P

F32 = jnp.float32
BF16 = jnp.bfloat16
MESH = pl.DeviceIdType.MESH


def rotate(values, position):
    half_dim = values.shape[-1] // 2
    freqs = 10000.0 ** (-jnp.arange(half_dim, dtype=jnp.float32) / half_dim)
    angles = position.astype(jnp.float32)[..., None] * freqs
    cosine = jnp.cos(angles)
    sine = jnp.sin(angles)
    first_half = values[..., :half_dim].astype(jnp.float32)
    second_half = values[..., half_dim:].astype(jnp.float32)
    return jnp.concatenate(
        [first_half * cosine - second_half * sine, second_half * cosine + first_half * sine],
        axis=-1,
    )


def mega(sz, qn_in, qr_in, kv_in, kr_in, pos_in, wuk_in, wuv_in, wout_in, out_ref,
         qn, qr, kv, kr, pos, wuk, wuv, wout, krot, table, limit, ho, acc, part, got,
         s_w, s_q, s_k, r_w, r_q, r_k, r_p, s_y, r_y, s_t, r_t, s_ag, r_ag, s_rs, r_rs, hop, loc_out):
    n, groups, tps, ends, mids = sz["n"], sz["g"], sz["t"], sz["ends"], sz["mids"]
    tok, hc, nope, rope, lat, vdim = (sz[k] for k in ("tok", "hc", "nope", "rope", "lat", "vdim"))
    scale = (nope + rope) ** (-0.5)
    hg = hc // groups
    c = lax.axis_index("ctx")
    g = lax.axis_index("groups")
    t = lax.axis_index("tp")
    nsl = nope // n
    lsl = lat // n
    share = tok // tps
    seq = n * tok

    def outer(j):
        return jnp.logical_or(j == 0, j == n - 1)

    def count(j):
        return jnp.where(outer(j), ends, mids)

    def begin(j):
        return jnp.where(j == 0, 0, ends + (j - 1) * mids)

    mine = count(c)
    first_mine = begin(c)
    at_end = outer(c)

    def al(x, m):
        return pl.multiple_of(x, m)

    def guard(i, j, body):
        if i < ends:
            body()
        else:
            pl.when(jnp.logical_not(outer(j)))(body)

    def rows_of(s):
        return pl.ds(al(s * tok, tok), tok)

    def piece(kind, i, j, s, part_of):
        if kind in (0, 5):
            src, dst = (kv_in, kv) if kind == 0 else (kr_in, kr)
            if part_of is None:
                return src, dst.at[rows_of(s), :]
            return (src.at[pl.ds(al(part_of * share, share), share), :],
                    dst.at[pl.ds(al(s * tok + part_of * share, share), share), :])
        if kind == 6:
            return pos_in, pos.at[s]
        if kind == 1:
            w = hc * nope
            return (qn_in.at[:, pl.ds(al((begin(j) + i) * w, w), w)],
                    qn.at[rows_of(s), pl.ds(i * w, w)])
        if kind == 2:
            w = hc * rope
            return (qr_in.at[:, pl.ds(al((begin(j) + i) * w, w), w)],
                    qr.at[rows_of(s), pl.ds(i * w, w)])
        if part_of is None:
            src_h, dst_h = pl.ds((begin(j) + i) * hc, hc), pl.ds(i * hc, hc)
        else:
            src_h = pl.ds((begin(j) + i) * hc + part_of * hg, hg)
            dst_h = pl.ds(i * hc + part_of * hg, hg)
        if kind == 3:
            return wuk_in.at[src_h], wuk.at[dst_h, pl.ds(al(s * nsl, nsl), nsl), :]
        return wuv_in.at[src_h], wuv.at[dst_h, pl.ds(al(s * lsl, lsl), lsl), :]

    def copy1(kind, i, d, to=None):
        owner = t if kind in (0, 5) else g
        if to is not None:
            j = to
            src, dst = piece(kind, i, j, c, owner)
        else:
            j = lax.rem(c + n - d, n)
            src, dst = piece(kind, i, c, j, owner)
        if kind in (3, 4):
            send, recv = s_w.at[i], r_w.at[i, d - 1]
        elif kind in (1, 2):
            send, recv = s_q.at[i], r_q.at[i]
        elif kind == 6:
            send, recv = s_k.at[2], r_p
        else:
            send, recv = s_k.at[kind // 5], r_k.at[kind // 5, d - 1]
        return pltpu.make_async_remote_copy(
            src_ref=src, dst_ref=dst, send_sem=send, recv_sem=recv,
            device_id={"ctx": j}, device_id_type=MESH)

    def local(kind, i):
        src, dst = piece(kind, i, c, c, None)
        if kind in (3, 4):
            sem = r_y.at[i]
        elif kind in (1, 2):
            sem = r_q.at[i]
        else:
            sem = r_p if kind == 6 else r_t.at[kind // 5]
        return pltpu.make_async_copy(src, dst, sem)

    def take(ref, sem):
        pltpu.make_async_copy(ref, ref, sem).wait()

    def weight_bytes(blocks):
        return wuk.at[pl.ds(0, blocks), pl.ds(0, nsl), :]

    def query_bytes(blocks):
        return qn.at[pl.ds(0, blocks * tok), pl.ds(0, hc * (nope + rope))]

    def key_bytes(kind, rows):
        return (kr if kind else kv).at[pl.ds(0, rows), :]

    def kinds(i):
        return (0, 1, 2, 3, 4, 5, 6) if i == 0 else (1, 2, 3, 4)

    def turn_of(i, total):
        groups_of = [((3, 4), 0)] if i == 0 else []
        if i + 1 < total:
            groups_of.append(((3, 4), i + 1))
        return groups_of + [((1, 2), i)]

    def send_chunk(b, i, total, targets):
        for group, k in turn_of(i, total):
            for j in targets:
                for kind in group:
                    copy1(kind, k, (j - b) % n, j).start()

    sides = (0, n - 1)

    def send_far_chunk(b, k, far):
        for kind in (3, 4, 1, 2):
            copy1(kind, k, (far - b) % n, far).start()

    for i in range(mids):
        def go():
            for kind in kinds(i):
                local(kind, i).start()
        guard(i, c, go)
    wout_copy = pltpu.make_async_copy(wout_in, wout, loc_out)
    wout_copy.start()

    barrier = pltpu.get_barrier_semaphore()

    def tell(sem, axis, to):
        pl.semaphore_signal(sem, inc=1, device_id={axis: to}, device_id_type=MESH)

    pl.when(c > 0)(lambda: tell(barrier, "ctx", c - 1))
    pl.when(c + 1 < n)(lambda: tell(barrier, "ctx", c + 1))
    for axis, me, size in (("groups", g, groups), ("tp", t, tps)):
        for d in range(1, size):
            tell(barrier, axis, lax.rem(me + d, size))
    pl.semaphore_wait(barrier, jnp.where(at_end, 1, 2) + (groups - 1) + (tps - 1))

    def send_keys(b, j, group):
        for kind in group:
            copy1(kind, 0, (j - b) % n, j).start()

    for b in range(n):
        @pl.when(c == b)
        def _():
            step = 1 if b < n // 2 else -1
            if b in sides:
                near, next_on, far = (b + k * step for k in range(1, n))
                middle = [next_on, near]
                send_keys(b, near, (6, 0, 5))
                pl.semaphore_wait(hop.at[0], 1)
                send_keys(b, next_on, (6, 0, 5))
                send_chunk(b, 0, mids, middle)
                pl.semaphore_wait(hop.at[1], 1)
                send_keys(b, far, (6,))
            else:
                outside, middle, far = b - step, [b + step], b + 2 * step
                for j in (outside, *middle):
                    tell(hop.at[0], "ctx", j)
                send_keys(b, middle[0], (6, 0, 5))
                send_chunk(b, 0, mids, middle)
                send_keys(b, outside, (6, 0, 5))
                for i in range(ends):
                    send_chunk(b, i, ends, [outside])
                pl.semaphore_wait(hop.at[0], 1)
                tell(hop.at[1], "ctx", outside)
                send_keys(b, far, (6,))
            for i in range(1, mids):
                send_chunk(b, i, mids, middle)
                if b not in sides:
                    for k in range(ends):
                        if i == mids - 1 - (ends - 1 - k) * sz["spread"]:
                            send_far_chunk(b, k, far)

    def send_far(k):
        for b in sides:
            pl.when(c == b)(functools.partial(send_far_chunk, b, k, n - 1 - b))

    def copy_y(kind, i, e, d, sending):
        s = lax.rem(c + n - d, n)
        owner = g if sending else lax.rem(g + groups - e, groups)
        _, dst = piece(kind, i, c, s, owner)
        to = lax.rem(g + e, groups) if sending else owner
        return pltpu.make_async_remote_copy(
            src_ref=dst, dst_ref=dst, send_sem=s_y.at[i], recv_sem=r_y.at[i],
            device_id={"groups": to}, device_id_type=MESH)

    def copy_t(kind, e, d, sending):
        s = lax.rem(c + n - d, n)
        owner = t if sending else lax.rem(t + tps - e, tps)
        _, dst = piece(kind, 0, c, s, owner)
        to = lax.rem(t + e, tps) if sending else owner
        return pltpu.make_async_remote_copy(
            src_ref=dst, dst_ref=dst, send_sem=s_t.at[kind // 5], recv_sem=r_t.at[kind // 5],
            device_id={"tp": to}, device_id_type=MESH)

    def forward_from(i, d):
        take(weight_bytes(2 * hg), r_w.at[i, d - 1])
        for kind in (3, 4):
            for e in range(1, groups):
                copy_y(kind, i, e, d, True).start()

    def forward_weights(i):
        @pl.when(jnp.logical_not(at_end))
        def _():
            forward_from(i, 3)
            forward_from(i, 1)

        forward_from(i, 2)

    def forward_others(near, far):
        for d in (near, far):
            for i in range(ends):
                forward_from(i, d)

    def pass_key(kind, b, origin, out):
        ref = (kr if kind else kv).at[pl.ds(al(origin * tok + t * share, share), share), :]
        return pltpu.make_async_remote_copy(
            src_ref=ref, dst_ref=ref, send_sem=s_k.at[kind // 5],
            recv_sem=r_k.at[kind // 5, (out - origin) % n - 1],
            device_id={"ctx": out}, device_id_type=MESH)

    def forward_keys():
        for d in range(1, n):
            for kind in (0, 5):
                copy1(kind, 0, d).wait_recv()
                for b in range(1, n - 1):
                    out = 0 if b < n // 2 else n - 1
                    if (b - d) % n != out:
                        pl.when(c == b)(lambda: pass_key(kind, b, (b - d) % n, out).start())
                for e in range(1, tps):
                    copy_t(kind, e, d, True).start()

    wide = 2 * rope

    def turn(x):
        lane = lax.broadcasted_iota(jnp.int32, x.shape, 1)
        low = lax.rem(lane, rope) < rope // 2
        other = jnp.where(low, -pltpu.roll(x, wide - rope // 2, 1), pltpu.roll(x, rope // 2, 1))
        return x * table[0] + other * table[1]

    def tables():
        take(pos, r_p)
        row = jnp.concatenate([pos[s] for s in range(n)], axis=1).astype(F32)
        col = jnp.broadcast_to(row, (wide, seq)).T
        lane = lax.broadcasted_iota(jnp.int32, (1, wide), 1)
        index = lax.rem(lane, rope // 2).astype(F32)
        freqs = jnp.exp(index * (-math.log(10000.0) / (rope // 2)))
        angles = col * freqs
        table[0] = jnp.cos(angles)
        table[1] = jnp.sin(angles)
        limit[...] = jnp.where(row > col[:, :1], -1e30, 3e38)

    def keys():
        for kind in (0, 5):
            take(key_bytes(kind, tok + (n - 1) * (tps - 1) * share), r_t.at[kind // 5])
        raw = kr[...].astype(F32)
        turned = turn(jnp.concatenate([raw, raw], axis=1))
        lane = lax.broadcasted_iota(jnp.int32, turned.shape, 1)
        krot[0] = jnp.where(lane < rope, turned, 0.0).astype(BF16)
        krot[1] = jnp.where(lane < rope, 0.0, turned).astype(BF16)

    def attend(i):
        nt = (((1,), (1,)), ((), ()))

        def pair(p, carry):
            raw = qr[:, pl.ds(al((i * (hc // 2) + p) * wide, wide), wide)]
            qrp = turn(raw.astype(F32)).astype(BF16)
            for k in range(2):
                hl = 2 * p + k
                h = i * hc + hl
                q = qn[:, pl.ds(al(h * nope, nope), nope)]
                ql = jnp.dot(q, wuk[h], preferred_element_type=F32).astype(BF16)
                sc = lax.dot_general(ql, kv[...], nt, preferred_element_type=F32)
                sc = (sc + lax.dot_general(qrp, krot[k], nt, preferred_element_type=F32)) * scale
                sc = jnp.minimum(sc, limit[...])
                w = jnp.exp(sc - jnp.max(sc, axis=1, keepdims=True))
                total = jnp.sum(w, axis=1, keepdims=True)
                o = jnp.dot(w.astype(BF16), kv[...], preferred_element_type=F32)
                o = (o / total).astype(BF16)
                ho[first_mine + i, :, pl.ds(al(hl * vdim, vdim), vdim)] = jnp.dot(
                    o, wuv[h], preferred_element_type=F32).astype(BF16)
            return carry

        lax.fori_loop(0, hc // 2, pair, 0)

    away, stay = 0, 1
    half_rows = seq // 2
    side = t // 2

    def rows_half(h):
        return pl.ds(al((1 - side if h == away else side) * half_rows, half_rows), half_rows)

    quarter = half_rows // 2

    def parts_of(h):
        return (0,) if h == away else (1, 2)

    def ag_copy(q, p, right):
        rows = rows_half(away)
        if p > 0:
            rows = pl.ds(al(side * half_rows + (p - 1) * quarter, quarter), quarter)
        ref = ho.at[q, rows, :]
        return pltpu.make_async_remote_copy(
            src_ref=ref, dst_ref=ref, send_sem=s_ag.at[1 if right else 0],
            recv_sem=r_ag.at[q, p],
            device_id={"ctx": c + 1 if right else c - 1}, device_id_type=MESH)

    inner_right = c < n // 2

    def send_item(i, h, right):
        for p in parts_of(h):
            ag_copy(first_mine + i, p, right).start()

    def send_inward(i, h):
        pl.when(inner_right)(functools.partial(send_item, i, h, True))
        pl.when(jnp.logical_not(inner_right))(functools.partial(send_item, i, h, False))

    def send_outward(i, h):
        pl.when(jnp.logical_and(inner_right, c > 0))(functools.partial(send_item, i, h, False))
        pl.when(jnp.logical_and(jnp.logical_not(inner_right), c + 1 < n))(
            functools.partial(send_item, i, h, True))

    cols = acc.shape[1]
    tile = sz["tile"]
    kdim = hc * vdim

    def project(q, rows):
        depth = pl.ds(al(q * kdim, kdim), kdim)

        def step(j, carry):
            at = pl.ds(al(j * tile, tile), tile)
            value = jnp.dot(ho[q, rows, :], wout[depth, at], preferred_element_type=F32)
            acc[rows, at] = acc[rows, at] + value
            return carry

        lax.fori_loop(0, cols // tile, step, 0)

    def arrive(b, i, h, right):
        @pl.when(jnp.logical_and(jnp.logical_and(b >= 0, b < n), jnp.logical_and(i >= 0, i < count(b))))
        def _():
            q = begin(b) + i
            more = c + 1 < n if right else c > 0
            for p in parts_of(h):
                with jax.named_scope("take"):
                    ag_copy(q, p, right).wait_recv()
                pl.when(more)(lambda: ag_copy(q, p, right).start())
            project(q, rows_half(h))

    def arrive_all(d, low, high, h):
        def body(i, carry):
            arrive(c + d, i, h, False)
            arrive(c - d, i, h, True)
            return carry

        lax.fori_loop(low, high, body, 0)

    def arrive_inward(i, h):
        pl.when(inner_right)(lambda: arrive(c + 1, i, h, False))
        pl.when(jnp.logical_not(inner_right))(lambda: arrive(c - 1, i, h, True))

    def arrive_outward(i, h):
        pl.when(inner_right)(lambda: arrive(c - 1, i, h, True))
        pl.when(jnp.logical_not(inner_right))(lambda: arrive(c + 1, i, h, False))

    early = sz["early"]

    def chunk(i):
        take(query_bytes(n), r_q.at[i])
        take(weight_bytes((n - 1) * (groups - 1) * 2 * hg + 2 * hc), r_y.at[i])
        attend(i)
        send_outward(i, away)
        send_inward(i, away)
        send_outward(i, stay)
        if i < early:
            pl.when(jnp.logical_not(at_end))(functools.partial(send_inward, i, stay))
        project(first_mine + i, slice(None))

    forward_keys()
    def between():
        tables()
        keys()
        acc[...] = jnp.zeros_like(acc)
        wout_copy.wait()

    @pl.when(jnp.logical_not(at_end))
    def _():
        forward_weights(0)
        between()

    @pl.when(at_end)
    def _():
        between()
        for i in range(sz["release"]):
            arrive_inward(i, away)
            arrive_inward(i, stay)
            for k in range(ends):
                if i == sz["release"] - 1 - (ends - 1 - k) * sz["gap"]:
                    send_far(k)
        pl.when(c == 0)(functools.partial(forward_others, 3, 1))
        pl.when(c == n - 1)(functools.partial(forward_others, 1, 3))
        forward_weights(0)

    for i in range(mids):
        if i + 1 < mids:
            guard(i + 1, c, functools.partial(forward_weights, i + 1))
        guard(i, c, functools.partial(chunk, i))

    def send_late(low, high):
        for i in range(low, high):
            send_inward(i, stay)

    pl.when(at_end)(functools.partial(send_late, 0, ends))
    @pl.when(jnp.logical_not(at_end))
    def _():
        for i in range(early):
            arrive_inward(i, away)
            arrive_inward(i, stay)

    seen = jnp.where(at_end, sz["release"], early)

    def first_away(i, carry):
        arrive_inward(i + seen, away)
        arrive_outward(i - sz["behind"], away)
        return carry

    lax.fori_loop(0, mids + sz["behind"], first_away, 0)
    pl.when(jnp.logical_not(at_end))(functools.partial(send_late, early, mids))

    rows_out = out_ref.shape[0]
    half = cols // 2
    core = lax.rem(t, 2)
    mate = t + 1 - 2 * core
    across = lax.rem(t + 2, tps)
    mate_across = lax.rem(mate + 2, tps)

    def block(r, at):
        return acc[pl.ds(al(r * rows_out, rows_out), rows_out), at]

    def rs_copy(stage, k):
        at = pl.ds(k * half, half)
        slot = (1, 2, 0)[stage]
        return pltpu.make_async_remote_copy(
            src_ref=part.at[slot, :, at], dst_ref=got.at[slot, :, at],
            send_sem=s_rs, recv_sem=r_rs.at[stage, k],
            device_id={"tp": across if stage == 1 else mate}, device_id_type=MESH)

    spans = [slice(k * half, (k + 1) * half) for k in range(2)]

    arrive_all(2, 0, mids, away)
    for i in range(mids):
        guard(i, c, lambda: take(weight_bytes((n - 1) * (groups - 1) * 2 * hg), s_y.at[i]))
    arrive_all(3, 0, ends, away)
    for k, at in enumerate(spans):
        part[1, :, at] = block(mate_across, at).astype(BF16)
        rs_copy(0, k).start()
    arrive_inward(seen, stay)
    arrive_outward(0, stay)
    for k, at in enumerate(spans):
        rs_copy(0, k).wait_recv()
        part[2, :, at] = (block(across, at) + got[1, :, at].astype(F32)).astype(BF16)
        rs_copy(1, k).start()

    def first_stay(i, carry):
        arrive_inward(i + seen, stay)
        arrive_outward(i, stay)
        return carry

    lax.fori_loop(1, mids, first_stay, 0)
    def sent(i, peers):
        take(weight_bytes(peers * 2 * hg), s_w.at[i])
        take(query_bytes(peers), s_q.at[i])

    for i in range(mids):
        if i < ends:
            sent(i, n - 1)
        else:
            pl.when(at_end)(functools.partial(sent, i, n - 2))
            pl.when(jnp.logical_not(at_end))(functools.partial(sent, i, n - 3))
    for kind in (0, 5):
        pl.when(at_end)(lambda: take(key_bytes(kind, 2 * share), s_k.at[kind // 5]))
        pl.when(jnp.logical_not(at_end))(lambda: take(key_bytes(kind, 4 * share), s_k.at[kind // 5]))
        take(key_bytes(kind, (n - 1) * (tps - 1) * share), s_t.at[kind // 5])
    take(pos.at[pl.ds(0, n - 1)], s_k.at[2])
    arrive_all(2, 0, mids, stay)

    def drain():
        for b in range(n):
            low = 0 if b == 0 else ends + (b - 1) * mids
            high = low + (ends if b in (0, n - 1) else mids)

            @pl.when(c == b)
            def _():
                if b + 1 < n:
                    take(ho.at[pl.ds(0, high)], s_ag.at[1])
                if b > 0:
                    take(ho.at[pl.ds(low, ho.shape[0] - low)], s_ag.at[0])

    arrive_all(3, 0, ends, stay)
    for k, at in enumerate(spans):
        part[0, :, at] = block(mate, at).astype(BF16)
        rs_copy(2, k).start()
    drain()
    for k, at in enumerate(spans):
        rs_copy(1, k).wait_recv()
        own = block(t, at) + got[2, :, at].astype(F32)
        rs_copy(2, k).wait_recv()
        out_ref[:, at] = (own + got[0, :, at].astype(F32)).astype(BF16)
    take(part, s_rs)


def fast(sz, q_nope, q_rope, c_kv, k_rope, positions, w_uk, w_uv, w_out):
    n, groups, tps, ends, mids = sz["n"], sz["g"], sz["t"], sz["ends"], sz["mids"]
    tok, hc, nope, rope, lat, vdim = (sz[k] for k in ("tok", "hc", "nope", "rope", "lat", "vdim"))
    heads = w_uk.shape[0]
    chunks = heads // hc
    hpc = mids * hc
    seq = n * tok
    cols = w_out.shape[1]
    hbm = pl.BlockSpec(memory_space=pltpu.HBM)
    dma = pltpu.SemaphoreType.DMA
    return pl.pallas_call(
        functools.partial(mega, sz),
        out_shape=pltpu.VMEM((seq // tps, cols), BF16),
        in_specs=[hbm] * 8,
        out_specs=pl.BlockSpec(memory_space=pltpu.VMEM),
        scratch_shapes=[
            pltpu.VMEM((seq, hpc * nope), BF16),
            pltpu.VMEM((seq, hpc * rope), BF16),
            pltpu.VMEM((seq, lat), BF16),
            pltpu.VMEM((seq, rope), BF16),
            pltpu.VMEM((n, 1, tok), jnp.int32),
            pltpu.VMEM((hpc, nope, lat), BF16),
            pltpu.VMEM((hpc, lat, vdim), BF16),
            pltpu.VMEM(w_out.shape, BF16),
            pltpu.VMEM((2, seq, 2 * rope), BF16),
            pltpu.VMEM((2, seq, 2 * rope), F32),
            pltpu.VMEM((seq, seq), F32),
            pltpu.VMEM((chunks, seq, hc * vdim), BF16),
            pltpu.VMEM((seq, cols), F32),
            pltpu.VMEM((tps - 1, seq // tps, cols), BF16),
            pltpu.VMEM((tps - 1, seq // tps, cols), BF16),
            dma((mids,)),
            dma((mids,)),
            dma((3,)),
            dma((mids, n - 1)),
            dma((mids,)),
            dma((2, n - 1)),
            dma,
            dma((mids,)),
            dma((mids,)),
            dma((2,)),
            dma((2,)),
            dma((2,)),
            dma((chunks, 3)),
            dma,
            dma((3, 2)),
            pltpu.SemaphoreType.REGULAR((2,)),
            dma,
        ],
        compiler_params=pltpu.CompilerParams(collective_id=0, has_side_effects=True,
                                             vmem_limit_bytes=60 * 1024 * 1024),
    )(q_nope, q_rope, c_kv, k_rope, positions.reshape(1, tok), w_uk, w_uv, w_out)


def general(q_nope, q_rope, c_kv, k_rope, positions, w_uk, w_uv, w_out):
    tok_count = q_nope.shape[0]
    head_count = w_uk.shape[0]
    latent = c_kv.shape[1]
    up_key, up_value = (
        lax.all_gather(w_uk, "ctx", axis=1, tiled=True),
        lax.all_gather(w_uv, "ctx", axis=1, tiled=True),
    )
    nope_dim = up_key.shape[1]
    rope_dim = k_rope.shape[1]
    softmax_scale = (nope_dim + rope_dim) ** (-0.5)
    q_parts = q_nope.reshape(tok_count, head_count, nope_dim)
    q_lat = jnp.einsum("thn,hnl->thl", q_parts, up_key, preferred_element_type=jnp.float32).astype(
        jnp.bfloat16
    )
    q_rot = rotate(q_rope.reshape(tok_count, head_count, rope_dim), positions[:, None]).astype(
        jnp.bfloat16
    )
    k_rot = rotate(k_rope, positions).astype(jnp.bfloat16)
    key_rows = jnp.concatenate([c_kv, k_rot], axis=1)
    queries = jnp.concatenate([q_lat, q_rot], axis=2).reshape(
        tok_count * head_count, latent + rope_dim
    )
    query_pos = jnp.repeat(positions, head_count)
    row_total = tok_count * head_count
    key_part = lax.all_gather(key_rows, "ctx", axis=0, tiled=True)
    key_pos = lax.all_gather(positions, "ctx", axis=0, tiled=True)
    run_max = jnp.full((row_total,), -1e30, jnp.float32)
    scores = (
        jnp.einsum("rk,sk->rs", queries, key_part, preferred_element_type=jnp.float32)
        * softmax_scale
    )
    visible = key_pos[None, :] <= query_pos[:, None]
    new_max = jnp.maximum(run_max, jnp.max(jnp.where(visible, scores, -1e30), axis=1))
    weights = jnp.where(visible, jnp.exp(scores - new_max[:, None]), 0.0)
    new_sum = jnp.sum(weights, axis=1)
    added = jnp.dot(
        weights.astype(jnp.bfloat16), key_part[:, :latent], preferred_element_type=jnp.float32
    )
    o_lat = (added / new_sum[:, None]).astype(jnp.bfloat16).reshape(tok_count, head_count, latent)
    head_out = jnp.einsum("thl,hlv->thv", o_lat, up_value, preferred_element_type=jnp.float32)
    rows_out = head_out.astype(jnp.bfloat16).reshape(tok_count, -1)
    partial_value = jnp.dot(
        lax.all_gather(rows_out, "ctx", axis=0, tiled=True),
        w_out,
        preferred_element_type=jnp.float32,
    )
    summed = lax.psum_scatter(
        partial_value.astype(jnp.bfloat16), "tp", scatter_dimension=0, tiled=True
    )
    return summed


CHUNK_HEADS = 2
END_CHUNKS = 2
RELEASE = 4
SPREAD = 2
GAP = 2
EARLY = 1
BEHIND = 1


def on_device(sizes, *args):
    q_nope, q_rope, c_kv, k_rope, positions, w_uk, w_uv, w_out = args
    n, groups, tps = sizes["ctx"], sizes["groups"], sizes["tp"]
    heads = w_uk.shape[0]
    chunks = heads // CHUNK_HEADS
    ends = END_CHUNKS * chunks // 16
    mids = chunks // 2 - ends
    sz = dict(n=n, g=groups, t=tps, hc=CHUNK_HEADS, ends=ends, mids=mids, tok=q_nope.shape[0],
              release=RELEASE, spread=SPREAD, gap=GAP, early=EARLY, behind=BEHIND,
              nope=w_uk.shape[1] * n, rope=k_rope.shape[1], lat=c_kv.shape[1],
              vdim=w_uv.shape[2], tile=w_out.shape[1] // 2)
    seq = n * sz["tok"]
    cols = w_out.shape[1]
    fits = (
        n == 4
        and tps == 4
        and heads % (2 * CHUNK_HEADS) == 0
        and CHUNK_HEADS % groups == 0
        and groups == 2
        and mids >= ends > EARLY
        and mids > RELEASE > (ends - 1) * GAP
        and mids - 1 > (ends - 1) * SPREAD
        and mids >= n + 1
        and sz["nope"] == sz["vdim"]
        and seq <= 512
        and seq % (tps * 16) == 0
        and sz["tok"] % (tps * 16) == 0
        and sz["rope"] == 64
        and sz["nope"] % 128 == 0
        and sz["vdim"] % 128 == 0
        and sz["lat"] % 128 == 0
        and cols % 256 == 0
        and w_out.size * 2 + seq * cols * 8 <= 32 * 2**20
    )
    if fits:
        return fast(sz, *args)
    return general(*args)


def solution(mesh):
    in_specs = (
        P(("groups", "ctx"), "tp"),
        P(("groups", "ctx"), "tp"),
        P(("groups", "ctx"), None),
        P(("groups", "ctx"), None),
        P(("groups", "ctx")),
        P("tp", "ctx", None),
        P("tp", "ctx", None),
        P("tp", "ctx"),
    )
    out_specs = P(("groups", "tp"), "ctx")
    return jax.shard_map(
        functools.partial(on_device, dict(mesh.shape)),
        mesh=mesh, in_specs=in_specs, out_specs=out_specs, check_vma=False,
    )
```
